8 devices in a mesh: dp: 1 (over z), tp: 8 (over y, x, core).
Axes of the slice: x: 2, y: 2, z: 1, core: 2. Of those that a mesh axis runs over, the one named last changes fastest.
Arguments:
- hidden: bfloat16 [8, 9, 4096], P('dp')
- draft_ids: int32 [8, 8], P('dp')
- norm_gain: bfloat16 [4096], replicated
- head_w: bfloat16 [4096, 128256], P(None, 'tp')
Outputs:
- output 1: float32 [8, 8], P('dp')
- output 2: float32 [8, 9], P('dp')
- output 3: float32 [8, 9], P('dp')
All inputs are finite; a program needn't handle non-finite values.
Results may differ from the reference program's by a relative error of at most 0.001.
Values sent between devices are 32-bit elements.
A program may use at most 1 GiB of HBM per device.

```python
import jax
import jax.numpy as jnp
from jax import lax

DIM = 4096
VOCAB = 128256
BATCH = 8
DRAFTS = 8
NORM_EPS = 1e-5


def setup_inputs(seed: int = 0, part: int = 0) -> dict:
    root_key = jax.random.key(seed)
    shared_key, part_base = jax.random.split(root_key)
    part_key = jax.random.fold_in(part_base, part)
    key_x, key_d = jax.random.split(part_key)
    key_g, key_w, key_hot = jax.random.split(shared_key, 3)
    hidden = jax.random.normal(key_x, (BATCH, DRAFTS + 1, DIM), jnp.float32)
    draft_ids = jax.random.randint(key_d, (BATCH, DRAFTS), 0, VOCAB, jnp.int32)
    norm_gain = 1.0 + 0.2 * jax.random.normal(key_g, (DIM,), jnp.float32)
    hot_cols = jax.random.randint(key_hot, (VOCAB,), 0, 64, jnp.int32) == 0
    col_scale = jnp.where(hot_cols, 3.5, 2.0) * DIM ** -0.5
    head_w = jax.random.normal(key_w, (DIM, VOCAB), jnp.float32) * col_scale
    return {'hidden': hidden.astype(jnp.bfloat16), 'draft_ids': draft_ids, 'norm_gain': norm_gain.astype(jnp.bfloat16), 'head_w': head_w.astype(jnp.bfloat16)}


def rms_norm(hidden, norm_gain):
    wide_x = hidden.astype(jnp.float32)
    inv_rms = lax.rsqrt(jnp.mean(wide_x * wide_x, axis=-1, keepdims=True) + NORM_EPS)
    return (wide_x * inv_rms * norm_gain.astype(jnp.float32)).astype(jnp.bfloat16)


def reference(hidden, draft_ids, norm_gain, head_w):
    def one_sequence(seq_pair):
        seq_rows, seq_ids = seq_pair
        normed = rms_norm(seq_rows, norm_gain)
        logits = jnp.dot(normed, head_w, preferred_element_type=jnp.float32)
        row_max = jnp.max(logits, axis=-1)
        shifted = logits - row_max[:, None]
        exp_vals = jnp.exp(shifted)
        exp_sum = jnp.sum(exp_vals, axis=-1)
        weighted = jnp.sum(exp_vals * shifted, axis=-1)
        log_sum = jnp.log(exp_sum)
        log_norm = row_max + log_sum
        entropy = log_sum - weighted / exp_sum
        drafts = seq_ids.shape[0]
        picked = jnp.take_along_axis(logits[:drafts], seq_ids[:, None], axis=1)[:, 0]
        return picked - log_norm[:drafts], log_norm, entropy
    draft_logp, log_norm, entropy = lax.map(one_sequence, (hidden, draft_ids))
    return draft_logp, log_norm, entropy
```

```python
import functools

import jax
import jax.numpy as jnp
from jax import lax
from jax.experimental import pallas as pl
from jax.experimental.pallas import tpu as pltpu
from jax.sharding import PartitionSpec as P

NORM_EPS = 1e-5
MESH = pl.DeviceIdType.MESH
LANES = 128
SUBLANES = 8
BLOCK = 256
SLOTS = 16
UNROLL = 4


def merge(state, logits, wanted):
    row_max, exp_sum, weighted, picked = state
    tiles = logits.reshape(-1, SUBLANES, LANES)
    new_max = jnp.maximum(row_max, jnp.max(tiles, axis=0))
    drop = row_max - new_max
    scale = jnp.exp(drop)
    shifted = tiles - new_max[None]
    exp_vals = jnp.exp(shifted)
    weighted = scale * (weighted + drop * exp_sum) + jnp.sum(exp_vals * shifted, axis=0)
    exp_sum = scale * exp_sum + jnp.sum(exp_vals, axis=0)
    steps = lax.broadcasted_iota(jnp.int32, tiles.shape, 0) * SUBLANES
    picked = picked + jnp.sum(jnp.where(wanted[None] == steps, tiles, 0.0), axis=0)
    return new_max, exp_sum, weighted, picked


def kernel(n, x_hbm, ids_ref, gain_ref, w_hbm, logp_ref, norm_ref, ent_ref,
           x_ref, xt_ref, w_ref, stats_ref, x_sem, w_sem, send_sem, recv_sem):
    me = lax.axis_index('tp')
    group = lax.axis_index('dp')
    batch, drafts = ids_ref.shape
    positions = norm_ref.shape[1]
    rows = batch * positions
    cols, dim = w_hbm.shape
    full = cols // BLOCK
    tail = cols - full * BLOCK

    def fetch(block, slot, size=BLOCK):
        start = pl.multiple_of(block * BLOCK, BLOCK)
        return pltpu.make_async_copy(w_hbm.at[pl.ds(start, size)], w_ref.at[slot, pl.ds(0, size)], w_sem.at[slot])

    x_copy = pltpu.make_async_copy(x_hbm, x_ref, x_sem)
    x_copy.start()
    for b in range(SLOTS):
        fetch(b, b).start()

    barrier = pltpu.get_barrier_semaphore()
    for o in range(1, n):
        pl.semaphore_signal(barrier, inc=1, device_id=(group, lax.rem(me + o, n)), device_id_type=MESH)

    lane = lax.broadcasted_iota(jnp.int32, (batch, LANES), 1)
    sub = lax.broadcasted_iota(jnp.int32, (batch, LANES), 0)
    ids = ids_ref[...]
    spread = jnp.full((batch, LANES), 0, jnp.int32)
    for t in range(drafts):
        spread = jnp.where((lane // batch) == t, ids[:, t:t + 1], spread)
    spread = jnp.sum(jnp.where(lane % batch == sub, spread, 0), axis=0, keepdims=True)
    wanted = jnp.where(lane < batch * drafts, spread - me * cols - sub, -(1 << 29))

    x_copy.wait()
    total = jnp.zeros((rows, LANES), jnp.float32)
    for c in range(dim // LANES):
        wide = x_ref[:, c * LANES:(c + 1) * LANES].astype(jnp.float32)
        total = total + wide * wide
    inv_rms = lax.rsqrt(jnp.sum(total, axis=1, keepdims=True) / dim + NORM_EPS)
    pad = jnp.zeros((LANES - rows, LANES), jnp.float32)
    gain = gain_ref[...].astype(jnp.float32)
    for c in range(dim // LANES):
        wide = x_ref[:, c * LANES:(c + 1) * LANES].astype(jnp.float32)
        normed = wide * inv_rms * gain[c:c + 1, :]
        padded = jnp.concatenate([normed, pad], axis=0)
        xt_ref[c * LANES:(c + 1) * LANES, :] = padded.T.astype(jnp.bfloat16)

    def step(block, slot, state, first, size=BLOCK):
        fetch(block, slot, size).wait()
        logits = jnp.dot(w_ref[slot, :size], xt_ref[...], preferred_element_type=jnp.float32)
        if first:
            top = jnp.max(logits.reshape(-1, SUBLANES, LANES), axis=0)
            zero = jnp.zeros((SUBLANES, LANES), jnp.float32)
            state = (top, zero, zero, zero)
        return merge(state, logits, wanted - block * BLOCK)

    def again(block, slot):
        @pl.when(block + SLOTS < full)
        def _():
            fetch(block + SLOTS, slot).start()
        if tail:
            @pl.when(block + SLOTS == full)
            def _():
                fetch(full, slot, tail).start()

    state = step(0, 0, None, True)
    again(0, 0)
    head = 1
    trips = (full - head) // UNROLL

    def body(i, state):
        for u in range(UNROLL):
            block = head + i * UNROLL + u
            slot = lax.rem(block, SLOTS)
            state = step(block, slot, state, False)
            again(block, slot)
        return state

    state = lax.fori_loop(0, trips, body, state)
    for block in range(head + trips * UNROLL, full):
        state = step(block, block % SLOTS, state, False)
        if block + SLOTS <= full:
            again(block, block % SLOTS)
    if tail:
        state = step(full, full % SLOTS, state, False, tail)

    row_max, exp_sum, weighted, picked = state
    top = jnp.max(row_max, axis=0, keepdims=True)
    drop = row_max - top
    scale = jnp.exp(drop)
    mine = [top, jnp.sum(scale * exp_sum, axis=0, keepdims=True),
            jnp.sum(scale * (weighted + drop * exp_sum), axis=0, keepdims=True), jnp.sum(picked, axis=0, keepdims=True)]
    sub8 = lax.broadcasted_iota(jnp.int32, (SUBLANES, LANES), 0)
    packed = jnp.zeros((SUBLANES, LANES), jnp.float32)
    for k, v in enumerate(mine):
        packed = jnp.where(sub8 == k, v, packed)
    stats_ref[me] = packed
    pl.semaphore_wait(barrier, n - 1)
    copies = []
    for o in range(1, n):
        peer = lax.rem(me + o, n)
        copy = pltpu.make_async_remote_copy(
            src_ref=stats_ref.at[me], dst_ref=stats_ref.at[me], send_sem=send_sem.at[o], recv_sem=recv_sem.at[o],
            device_id=(group, peer), device_id_type=MESH)
        copy.start()
        copies.append(copy)
    for copy in copies:
        copy.wait()

    every = stats_ref[...]
    top = jnp.max(every[:, 0:1], axis=0)
    drop = every[:, 0:1] - top[None]
    scale = jnp.exp(drop)
    exp_sum = jnp.sum(scale * every[:, 1:2], axis=0)
    weighted = jnp.sum(scale * (every[:, 2:3] + drop * every[:, 1:2]), axis=0)
    picked = jnp.sum(every[:, 3:4], axis=0)
    log_sum = jnp.log(exp_sum)
    log_norm = top + log_sum
    entropy = log_sum - weighted / exp_sum
    logp = picked - log_norm

    def unspread(values, width):
        out = jnp.zeros((batch, LANES), jnp.float32)
        wide = jnp.broadcast_to(values, (batch, LANES))
        for t in range(width):
            out = jnp.where(lane == t, jnp.sum(jnp.where(lane == t * batch + sub, wide, 0.0), axis=1, keepdims=True), out)
        return out[:, :width]

    logp_ref[...] = unspread(logp, drafts)
    norm_ref[...] = unspread(log_norm, positions)
    ent_ref[...] = unspread(entropy, positions)


def solution(mesh):
    n = mesh.shape['tp']

    def per_device(hidden, draft_ids, norm_gain, head_w):
        batch, positions, dim = hidden.shape
        drafts = draft_ids.shape[1]
        rows = batch * positions
        x = hidden.transpose(1, 0, 2).reshape(rows, dim)
        gain = norm_gain.reshape(dim // LANES, LANES)
        vmem = pl.BlockSpec(memory_space=pltpu.VMEM)
        hbm = pl.BlockSpec(memory_space=pltpu.HBM)
        return pl.pallas_call(
            functools.partial(kernel, n),
            out_shape=(jax.ShapeDtypeStruct((batch, drafts), jnp.float32),
                       jax.ShapeDtypeStruct((batch, positions), jnp.float32),
                       jax.ShapeDtypeStruct((batch, positions), jnp.float32)),
            in_specs=[hbm, vmem, vmem, hbm],
            out_specs=(vmem, vmem, vmem),
            scratch_shapes=[
                pltpu.VMEM((rows, dim), jnp.bfloat16),
                pltpu.VMEM((dim, LANES), jnp.bfloat16),
                pltpu.VMEM((SLOTS, BLOCK, dim), jnp.bfloat16),
                pltpu.VMEM((n, SUBLANES, LANES), jnp.float32),
                pltpu.SemaphoreType.DMA,
                pltpu.SemaphoreType.DMA((SLOTS,)),
                pltpu.SemaphoreType.DMA((n,)),
                pltpu.SemaphoreType.DMA((n,)),
            ],
            compiler_params=pltpu.CompilerParams(collective_id=0, has_side_effects=True, vmem_limit_bytes=60 * 1024 * 1024),
        )(x, draft_ids, gain, head_w.T)

    specs_in = (P('dp', None, None), P('dp', None), P(None), P(None, 'tp'))
    specs_out = (P('dp', None), P('dp', None), P('dp', None))
    return jax.shard_map(per_device, mesh=mesh, in_specs=specs_in, out_specs=specs_out, check_vma=False)
```

```python
import functools

import jax
import jax.numpy as jnp
from jax import lax
from jax.experimental import pallas as pl
from jax.experimental.pallas import tpu as pltpu
from jax.sharding import PartitionSpec as P

NORM_EPS = 1e-5
MESH = pl.DeviceIdType.MESH
LANES = 128
SUBLANES = 8
UNIT = 256
PACK = 16
HELD = 256
MOVED = 304
UNITS = 2
TRIP = UNITS * (HELD + MOVED)
SLOTS = 5
CUTS = 4
FIELD = 16


def fold(state, tiles, hits, start):
    row_max, exp_sum, weighted, picked = state
    base = row_max if start is None else jnp.where(start, tiles[0], row_max)
    new_max = functools.reduce(jnp.maximum, tiles, base)
    drop = base - new_max
    scale = jnp.exp(drop)
    weighted = scale * (weighted + drop * exp_sum)
    exp_sum = scale * exp_sum
    for tile, hit in zip(tiles, hits):
        shifted = tile - new_max
        exp_vals = jnp.exp(shifted)
        exp_sum = exp_sum + exp_vals
        weighted = weighted + exp_vals * shifted
        picked = picked + jnp.where(hit, tile, 0.0)
    return new_max, exp_sum, weighted, picked


def score(x_hbm, ids_ref, gain_ref, w_hbm, stats_ref,
          x_ref, n_ref, xt_ref, w_ref, edge_ref, state_ref, x_sem, w_sem, edge_sem, cut_sem):
    me = lax.axis_index('tp')
    batch, drafts = ids_ref.shape
    rows = x_hbm.shape[0]
    positions = rows // batch
    cols, dim = w_hbm.shape
    depth = dim // UNIT
    trips = cols // TRIP
    edge = cols - trips * TRIP
    cut = dim // CUTS

    def fetch(trip, slot):
        start = pl.multiple_of(edge + trip * TRIP, SUBLANES)
        return pltpu.make_async_copy(w_hbm.at[pl.ds(start, TRIP)], w_ref.at[slot], w_sem.at[slot])

    def fetch_cut(c):
        part = pl.ds(c * cut, cut)
        return pltpu.make_async_copy(w_hbm.at[pl.ds(cols - TRIP, TRIP), part], w_ref.at[(trips - 1) % SLOTS, :, part], cut_sem.at[c])

    x_copy = pltpu.make_async_copy(x_hbm, x_ref, x_sem)
    x_copy.start()
    edge_copy = pltpu.make_async_copy(w_hbm.at[pl.ds(0, edge)], edge_ref, edge_sem)
    edge_copy.start()
    for b in range(SLOTS):
        fetch(b, b).start()

    lane = lax.broadcasted_iota(jnp.int32, (SUBLANES, LANES), 1)
    sub = lax.broadcasted_iota(jnp.int32, (SUBLANES, LANES), 0)
    ids = ids_ref[...] - me * cols
    nobody = jnp.full((SUBLANES, LANES), -(1 << 29), jnp.int32)
    wide_ids = [ids[:, t:t + 1] - lane for t in range(drafts)] + [nobody] * (positions - drafts)
    tall_ids = nobody
    for t in range(drafts):
        spread = jnp.sum(jnp.where(lane == t * batch + sub, ids[:, t:t + 1], 0), axis=0, keepdims=True)
        tall_ids = jnp.where(lane // batch == t, spread - sub, tall_ids)

    x_copy.wait()
    total = jnp.zeros((rows, LANES), jnp.float32)
    for c in range(dim // LANES):
        wide = x_ref[:, c * LANES:(c + 1) * LANES].astype(jnp.float32)
        total = total + wide * wide
    inv_rms = lax.rsqrt(jnp.sum(total, axis=1, keepdims=True) / dim + NORM_EPS)
    gain = gain_ref[...].astype(jnp.float32)
    pad = jnp.zeros((LANES - rows, LANES), jnp.float32)
    for c in range(dim // LANES):
        wide = x_ref[:, c * LANES:(c + 1) * LANES].astype(jnp.float32)
        normed = jnp.concatenate([wide * inv_rms * gain[c:c + 1, :], pad], axis=0)
        n_ref[:, c * LANES:(c + 1) * LANES] = normed[:n_ref.shape[0]].astype(jnp.bfloat16)
        xt_ref[c * LANES:(c + 1) * LANES, :] = normed.T.astype(jnp.bfloat16)

    zeros = jnp.zeros((UNIT, UNIT - LANES), jnp.bfloat16)

    def hold_x(k, q):
        pltpu.matmul_push_rhs(jnp.concatenate([xt_ref[k * UNIT:(k + 1) * UNIT, :], zeros], axis=1), staging_register=1, mxu_index=q)

    def tall_tiles(logits):
        return [logits[r:r + SUBLANES, :LANES] for r in range(0, logits.shape[0], SUBLANES)]

    def tall_hits(first_row, count):
        return [(tall_ids - first_row) == r * SUBLANES for r in range(count)]

    def main(held_0, held_1, moved_0, moved_1, edge_0, edge_1):
        held, moved, edges = (held_0, held_1), (moved_0, moved_1), (edge_0, edge_1)
        for ref in held + moved + edges:
            pltpu.matmul_pop(ref)

        half = edge // UNITS
        for q in range(UNITS):
            hold_x(0, q)
        edge_copy.wait()
        for k in range(depth):
            for q in range(UNITS):
                pltpu.matmul_acc_lhs(edges[q], edge_ref[q * half:(q + 1) * half, k * UNIT:(k + 1) * UNIT], load_staged_rhs=1)
                hold_x((k + 1) % depth, q)
        tiles, hits = [], []
        for q in range(UNITS):
            tiles += tall_tiles(pltpu.matmul_pop(edges[q]))
            hits += tall_hits(q * half, half // SUBLANES)
        zero = jnp.zeros((SUBLANES, LANES), jnp.float32)
        tall = fold((tiles[0], zero, zero, zero), tiles, hits, None)
        state_ref[...] = jnp.zeros_like(state_ref)

        def trip_step(trip, slot, tall, last):
            if not last:
                fetch(trip, slot).wait()
            first_row = edge + trip * TRIP
            for k in range(depth):
                if last and k % (depth // CUTS) == 0:
                    fetch_cut(k // (depth // CUTS)).wait()
                part = slice(k * UNIT, (k + 1) * UNIT)
                for q in range(UNITS):
                    top = q * (HELD + MOVED)
                    pltpu.matmul_push_rhs(w_ref[slot, top:top + HELD, part], staging_register=0, mxu_index=q, transpose=True)
                    pltpu.matmul_acc_lhs(moved[q], w_ref[slot, top + HELD:top + HELD + MOVED, part], load_staged_rhs=1)
                    if not (last and k == depth - 1):
                        hold_x((k + 1) % depth, q)
                    pltpu.matmul_acc_lhs(held[q], n_ref[:, part], load_staged_rhs=0)
            wide_tiles = []
            tiles, hits = [], []
            for q in range(UNITS):
                row = first_row + q * (HELD + MOVED)
                logits = pltpu.matmul_pop(moved[q])
                tiles += tall_tiles(logits)
                hits += tall_hits(row + HELD, MOVED // SUBLANES)
            tall = fold(tall, tiles, hits, None)
            for q in range(UNITS):
                row = first_row + q * (HELD + MOVED)
                logits = pltpu.matmul_pop(held[q])
                for c in range(HELD // LANES):
                    wide_tiles.append((logits[:, c * LANES:(c + 1) * LANES], row + c * LANES))
            for t in range(positions):
                here = slice(t * SUBLANES, (t + 1) * SUBLANES)
                state = tuple(state_ref[s, t] for s in range(4))
                state = fold(state, [z[here] for z, _ in wide_tiles], [wide_ids[t] == row for _, row in wide_tiles], trip == 0)
                for s in range(4):
                    state_ref[s, t] = state[s]
            return tall

        def body(trip, tall):
            slot = lax.rem(trip, SLOTS)
            tall = trip_step(trip, slot, tall, False)
            return tall

        def filling(trip, tall):
            tall = body(trip, tall)
            fetch(trip + SLOTS, lax.rem(trip, SLOTS)).start()
            return tall

        tall = lax.fori_loop(0, trips - 1 - SLOTS, filling, tall)
        tall = body(trips - 1 - SLOTS, tall)
        for c in range(CUTS):
            fetch_cut(c).start()
        tall = lax.fori_loop(trips - SLOTS, trips - 1, body, tall)
        tall = trip_step(trips - 1, (trips - 1) % SLOTS, tall, True)

        row_max, exp_sum, weighted, picked = tall
        top = jnp.max(row_max, axis=0, keepdims=True)
        drop = row_max - top
        scale = jnp.exp(drop)
        tall_row = [jnp.broadcast_to(v, (SUBLANES, LANES)) for v in (
            top, jnp.sum(scale * exp_sum, axis=0, keepdims=True),
            jnp.sum(scale * (weighted + drop * exp_sum), axis=0, keepdims=True), jnp.sum(picked, axis=0, keepdims=True))]
        packed = jnp.zeros((SUBLANES, LANES), jnp.float32)
        for t in range(positions):
            row_max, exp_sum, weighted, picked = (state_ref[s, t] for s in range(4))
            own = lane == t * batch + sub
            top = jnp.max(jnp.where(own, jnp.maximum(row_max, tall_row[0]), row_max), axis=1, keepdims=True)
            drop, far = row_max - top, jnp.where(own, tall_row[0] - top, 0.0)
            scale, other = jnp.exp(drop), jnp.exp(far)
            values = (top,
                      jnp.sum(scale * exp_sum + jnp.where(own, other * tall_row[1], 0.0), axis=1, keepdims=True),
                      jnp.sum(scale * (weighted + drop * exp_sum) + jnp.where(own, other * (tall_row[2] + far * tall_row[1]), 0.0), axis=1, keepdims=True),
                      jnp.sum(picked + jnp.where(own, tall_row[3], 0.0), axis=1, keepdims=True))
            for s, v in enumerate(values):
                packed = jnp.where(lane == s * FIELD + t, v, packed)
        stats_ref[...] = packed

    acc = pltpu.ACC
    f32 = jnp.float32
    pl.run_scoped(main, *[acc(q)((n_ref.shape[0], UNIT), f32) for q in range(UNITS)],
                  *[acc(q)((MOVED, UNIT), f32) for q in range(UNITS)],
                  *[acc(q)((edge // UNITS, UNIT), f32) for q in range(UNITS)])


def exchange(n, mine_ref, all_ref, send_sem, recv_sem):
    me = lax.axis_index('tp')
    group = lax.axis_index('dp')
    barrier = pltpu.get_barrier_semaphore()
    for o in range(1, n):
        pl.semaphore_signal(barrier, inc=1, device_id=(group, lax.rem(me + o, n)), device_id_type=MESH)
    all_ref[me] = mine_ref[...]
    pl.semaphore_wait(barrier, n - 1)
    copies = []
    for o in range(1, n):
        copy = pltpu.make_async_remote_copy(
            src_ref=mine_ref, dst_ref=all_ref.at[me], send_sem=send_sem.at[o], recv_sem=recv_sem.at[o],
            device_id=(group, lax.rem(me + o, n)), device_id_type=MESH)
        copy.start()
        copies.append(copy)
    for copy in copies:
        copy.wait()


def combine(n, all_ref, logp_ref, norm_ref, ent_ref):
    parts = [all_ref[d] for d in range(n)]
    fields = [[p if s == 0 else pltpu.roll(p, LANES - s * FIELD, 1) for p in parts] for s in range(4)]
    top = functools.reduce(jnp.maximum, fields[0])
    exp_sum = weighted = picked = jnp.zeros((SUBLANES, LANES), jnp.float32)
    for d in range(n):
        drop = fields[0][d] - top
        scale = jnp.exp(drop)
        exp_sum = exp_sum + scale * fields[1][d]
        weighted = weighted + scale * (fields[2][d] + drop * fields[1][d])
        picked = picked + fields[3][d]
    log_sum = jnp.log(exp_sum)
    log_norm = top + log_sum
    logp_ref[...] = (picked - log_norm)[:, :logp_ref.shape[1]]
    norm_ref[...] = log_norm[:, :norm_ref.shape[1]]
    ent_ref[...] = (log_sum - weighted / exp_sum)[:, :ent_ref.shape[1]]


def solution(mesh):
    n = mesh.shape['tp']

    def per_device(hidden, draft_ids, norm_gain, head_w):
        batch, positions, dim = hidden.shape
        drafts = draft_ids.shape[1]
        rows = batch * positions
        cols = head_w.shape[1]
        x = hidden.transpose(1, 0, 2).reshape(rows, dim)
        gain = norm_gain.reshape(dim // LANES, LANES)
        vmem = pl.BlockSpec(memory_space=pltpu.VMEM)
        hbm = pl.BlockSpec(memory_space=pltpu.HBM)
        tile = jax.ShapeDtypeStruct((SUBLANES, LANES), jnp.float32)
        mine = pl.pallas_call(
            score,
            out_shape=tile,
            in_specs=[hbm, vmem, vmem, hbm],
            out_specs=vmem,
            scratch_shapes=[
                pltpu.VMEM((rows, dim), jnp.bfloat16),
                pltpu.VMEM((pl.cdiv(rows, PACK) * PACK, dim), jnp.bfloat16),
                pltpu.VMEM((dim, LANES), jnp.bfloat16),
                pltpu.VMEM((SLOTS, TRIP, dim), jnp.bfloat16),
                pltpu.VMEM((cols % TRIP, dim), jnp.bfloat16),
                pltpu.VMEM((4, positions, SUBLANES, LANES), jnp.float32),
                pltpu.SemaphoreType.DMA,
                pltpu.SemaphoreType.DMA((SLOTS,)),
                pltpu.SemaphoreType.DMA,
                pltpu.SemaphoreType.DMA((CUTS,)),
            ],
            compiler_params=pltpu.CompilerParams(vmem_limit_bytes=60 * 1024 * 1024),
        )(x, draft_ids, gain, head_w.T)
        every = pl.pallas_call(
            functools.partial(exchange, n),
            out_shape=jax.ShapeDtypeStruct((n, SUBLANES, LANES), jnp.float32),
            in_specs=[vmem],
            out_specs=vmem,
            scratch_shapes=[pltpu.SemaphoreType.DMA((n,)), pltpu.SemaphoreType.DMA((n,))],
            compiler_params=pltpu.CompilerParams(collective_id=0, has_side_effects=True, vmem_limit_bytes=1024 * 1024),
        )(mine)
        return pl.pallas_call(
            functools.partial(combine, n),
            out_shape=(jax.ShapeDtypeStruct((batch, drafts), jnp.float32),
                       jax.ShapeDtypeStruct((batch, positions), jnp.float32),
                       jax.ShapeDtypeStruct((batch, positions), jnp.float32)),
            in_specs=[vmem],
            out_specs=(vmem, vmem, vmem),
            compiler_params=pltpu.CompilerParams(vmem_limit_bytes=1024 * 1024),
        )(every)

    specs_in = (P('dp', None, None), P('dp', None), P(None), P(None, 'tp'))
    specs_out = (P('dp', None), P('dp', None), P('dp', None))
    return jax.shard_map(per_device, mesh=mesh, in_specs=specs_in, out_specs=specs_out, check_vma=False)
```

```python
import functools

import jax
import jax.numpy as jnp
from jax import lax
from jax.experimental import pallas as pl
from jax.experimental.pallas import tpu as pltpu
from jax.sharding import PartitionSpec as P

NORM_EPS = 1e-5
MESH = pl.DeviceIdType.MESH
LANES = 128
SUBLANES = 8
UNIT = 256
PACK = 16
HELD = 256
MOVED = 304
UNITS = 2
TRIP = UNITS * (HELD + MOVED)
SLOTS = 4
CUTS = 8
SCORE_VMEM = 46 * 1024 * 1024
FIELD = 16


def fold(state, tiles, hits, start):
    row_max, exp_sum, weighted, picked = state
    base = row_max if start is None else jnp.where(start, tiles[0], row_max)
    new_max = functools.reduce(jnp.maximum, tiles, base)
    drop = base - new_max
    scale = jnp.exp(drop)
    weighted = scale * (weighted + drop * exp_sum)
    exp_sum = scale * exp_sum
    for tile, hit in zip(tiles, hits):
        shifted = tile - new_max
        exp_vals = jnp.exp(shifted)
        exp_sum = exp_sum + exp_vals
        weighted = weighted + exp_vals * shifted
        picked = picked + jnp.where(hit, tile, 0.0)
    return new_max, exp_sum, weighted, picked


def tall_tiles(logits):
    return [logits[r:r + SUBLANES, :LANES] for r in range(0, logits.shape[0], SUBLANES)]


def tall_hits(tall_ids, first_row, count):
    return [(tall_ids - first_row) == r * SUBLANES for r in range(count)]


def score(x_hbm, ids_hbm, gain_hbm, w_hbm, tall_ref, state_ref, ids_out, moved_ref, held_ref,
          x_ref, ids_ref, gain_ref, n_ref, xt_ref, w_ref, edge_ref, in_sem, w_sem, edge_sem, cut_sem):
    me = lax.axis_index('tp')
    batch, drafts = ids_ref.shape
    rows = x_hbm.shape[0]
    positions = rows // batch
    cols, dim = w_hbm.shape
    depth = dim // UNIT
    trips = cols // TRIP
    edge = cols - trips * TRIP
    cut = dim // CUTS

    def fetch(trip, slot):
        start = pl.multiple_of(edge + trip * TRIP, SUBLANES)
        return pltpu.make_async_copy(w_hbm.at[pl.ds(start, TRIP)], w_ref.at[slot], w_sem.at[slot])

    def fetch_cut(c):
        part = pl.ds(c * cut, cut)
        return pltpu.make_async_copy(w_hbm.at[pl.ds(cols - TRIP, TRIP), part], w_ref.at[(trips - 1) % SLOTS, :, part], cut_sem.at[c])

    inputs = [pltpu.make_async_copy(src, dst, in_sem.at[i])
              for i, (src, dst) in enumerate(((x_hbm, x_ref), (ids_hbm, ids_ref), (gain_hbm, gain_ref)))]
    for copy in inputs:
        copy.start()
    edge_copy = pltpu.make_async_copy(w_hbm.at[pl.ds(0, edge)], edge_ref, edge_sem)
    edge_copy.start()
    for b in range(SLOTS):
        fetch(b, b).start()

    lane = lax.broadcasted_iota(jnp.int32, (SUBLANES, LANES), 1)
    sub = lax.broadcasted_iota(jnp.int32, (SUBLANES, LANES), 0)
    for copy in inputs:
        copy.wait()
    ids = ids_ref[...] - me * cols
    nobody = jnp.full((SUBLANES, LANES), -(1 << 29), jnp.int32)
    wide_ids = [ids[:, t:t + 1] - lane for t in range(drafts)] + [nobody] * (positions - drafts)
    tall_ids = nobody
    for t in range(drafts):
        spread = jnp.sum(jnp.where(lane == t * batch + sub, ids[:, t:t + 1], 0), axis=0, keepdims=True)
        tall_ids = jnp.where(lane // batch == t, spread - sub, tall_ids)

    total = jnp.zeros((rows, LANES), jnp.float32)
    for c in range(dim // LANES):
        wide = x_ref[:, c * LANES:(c + 1) * LANES].astype(jnp.float32)
        total = total + wide * wide
    inv_rms = lax.rsqrt(jnp.sum(total, axis=1, keepdims=True) / dim + NORM_EPS)
    gain = gain_ref[...].astype(jnp.float32)
    pad = jnp.zeros((LANES - rows, LANES), jnp.float32)
    for c in range(dim // LANES):
        wide = x_ref[:, c * LANES:(c + 1) * LANES].astype(jnp.float32)
        normed = jnp.concatenate([wide * inv_rms * gain[c:c + 1, :], pad], axis=0)
        n_ref[:, c * LANES:(c + 1) * LANES] = normed[:n_ref.shape[0]].astype(jnp.bfloat16)
        xt_ref[c * LANES:(c + 1) * LANES, :] = normed.T.astype(jnp.bfloat16)

    zeros = jnp.zeros((UNIT, UNIT - LANES), jnp.bfloat16)

    def hold_x(k, q):
        pltpu.matmul_push_rhs(jnp.concatenate([xt_ref[k * UNIT:(k + 1) * UNIT, :], zeros], axis=1), staging_register=1, mxu_index=q)

    for t in range(positions):
        ids_out[t] = wide_ids[t]
    ids_out[positions] = tall_ids

    def main(held_0, held_1, moved_0, moved_1, edge_0, edge_1):
        held, moved, edges = (held_0, held_1), (moved_0, moved_1), (edge_0, edge_1)
        for ref in held + moved + edges:
            pltpu.matmul_pop(ref)

        half = edge // UNITS
        for q in range(UNITS):
            hold_x(0, q)
        edge_copy.wait()
        for k in range(depth):
            for q in range(UNITS):
                pltpu.matmul_acc_lhs(edges[q], edge_ref[q * half:(q + 1) * half, k * UNIT:(k + 1) * UNIT], load_staged_rhs=1)
                hold_x((k + 1) % depth, q)
        tiles, hits = [], []
        for q in range(UNITS):
            tiles += tall_tiles(pltpu.matmul_pop(edges[q]))
            hits += tall_hits(tall_ids, q * half, half // SUBLANES)
        zero = jnp.zeros((SUBLANES, LANES), jnp.float32)
        tall = fold((tiles[0], zero, zero, zero), tiles, hits, None)
        state_ref[...] = jnp.zeros_like(state_ref)

        def trip_step(trip, slot, tall, last):
            if not last:
                fetch(trip, slot).wait()
            first_row = edge + trip * TRIP
            for k in range(depth):
                if last and k % (depth // CUTS) == 0:
                    fetch_cut(k // (depth // CUTS)).wait()
                part = slice(k * UNIT, (k + 1) * UNIT)
                for q in range(UNITS):
                    top = q * (HELD + MOVED)
                    pltpu.matmul_push_rhs(w_ref[slot, top:top + HELD, part], staging_register=0, mxu_index=q, transpose=True)
                    pltpu.matmul_acc_lhs(moved[q], w_ref[slot, top + HELD:top + HELD + MOVED, part], load_staged_rhs=1)
                    if not (last and k == depth - 1):
                        hold_x((k + 1) % depth, q)
                    pltpu.matmul_acc_lhs(held[q], n_ref[:, part], load_staged_rhs=0)
            if last:
                for q in range(UNITS):
                    moved_ref[q] = pltpu.matmul_pop(moved[q])[:, :LANES]
                for q in range(UNITS):
                    held_ref[q] = pltpu.matmul_pop(held[q])
                return tall
            wide_tiles = []
            tiles, hits = [], []
            for q in range(UNITS):
                row = first_row + q * (HELD + MOVED)
                logits = pltpu.matmul_pop(moved[q])
                tiles += tall_tiles(logits)
                hits += tall_hits(tall_ids, row + HELD, MOVED // SUBLANES)
            tall = fold(tall, tiles, hits, None)
            for q in range(UNITS):
                row = first_row + q * (HELD + MOVED)
                logits = pltpu.matmul_pop(held[q])
                for c in range(HELD // LANES):
                    wide_tiles.append((logits[:, c * LANES:(c + 1) * LANES], row + c * LANES))
            for t in range(positions):
                here = slice(t * SUBLANES, (t + 1) * SUBLANES)
                state = tuple(state_ref[s, t] for s in range(4))
                state = fold(state, [z[here] for z, _ in wide_tiles], [wide_ids[t] == row for _, row in wide_tiles], trip == 0)
                for s in range(4):
                    state_ref[s, t] = state[s]
            return tall

        def body(trip, tall):
            slot = lax.rem(trip, SLOTS)
            tall = trip_step(trip, slot, tall, False)
            return tall

        def filling(trip, tall):
            tall = body(trip, tall)
            fetch(trip + SLOTS, lax.rem(trip, SLOTS)).start()
            return tall

        tall = lax.fori_loop(0, trips - 1 - SLOTS, filling, tall)
        tall = body(trips - 1 - SLOTS, tall)
        for c in range(CUTS):
            fetch_cut(c).start()
        tall = lax.fori_loop(trips - SLOTS, trips - 1, body, tall)
        tall = trip_step(trips - 1, (trips - 1) % SLOTS, tall, True)

        for s in range(4):
            tall_ref[s] = tall[s]

    acc = pltpu.ACC
    f32 = jnp.float32
    pl.run_scoped(main, *[acc(q)((n_ref.shape[0], UNIT), f32) for q in range(UNITS)],
                  *[acc(q)((MOVED, UNIT), f32) for q in range(UNITS)],
                  *[acc(q)((edge // UNITS, UNIT), f32) for q in range(UNITS)])


def exchange(n, last_row, tall_ref, state_ref, ids_ref, moved_ref, held_ref, all_ref, mine_ref, send_sem, recv_sem):
    me = lax.axis_index('tp')
    group = lax.axis_index('dp')
    batch, positions = SUBLANES, state_ref.shape[1]
    bits = [(d, lax.rem(me // d, 2)) for d in (1, 2, 4)]
    order = [o for o in (6, 7, 4, 5, 2, 3, 1) if o < n]
    peers = {o: me + sum(d * (1 - 2 * b) for d, b in bits if o & d) for o in order}
    barrier = pltpu.get_barrier_semaphore()
    for o in order:
        pl.semaphore_signal(barrier, inc=1, device_id=(group, peers[o]), device_id_type=MESH)

    lane = lax.broadcasted_iota(jnp.int32, (SUBLANES, LANES), 1)
    sub = lax.broadcasted_iota(jnp.int32, (SUBLANES, LANES), 0)
    tiles, hits = [], []
    for q in range(UNITS):
        row = last_row + q * (HELD + MOVED)
        tiles += tall_tiles(moved_ref[q])
        hits += tall_hits(ids_ref[positions], row + HELD, MOVED // SUBLANES)
    tall = fold(tuple(tall_ref[s] for s in range(4)), tiles, hits, None)
    wide = []
    for t in range(positions):
        tiles, hits = [], []
        for q in range(UNITS):
            for c in range(HELD // LANES):
                tiles.append(held_ref[q, t * SUBLANES:(t + 1) * SUBLANES, c * LANES:(c + 1) * LANES])
                hits.append(ids_ref[t] == last_row + q * (HELD + MOVED) + c * LANES)
        wide.append(fold(tuple(state_ref[s, t] for s in range(4)), tiles, hits, None))

    row_max, exp_sum, weighted, picked = tall
    top = jnp.max(row_max, axis=0, keepdims=True)
    drop = row_max - top
    scale = jnp.exp(drop)
    flat = [jnp.broadcast_to(v, (SUBLANES, LANES)) for v in (
        top, jnp.sum(scale * exp_sum, axis=0, keepdims=True),
        jnp.sum(scale * (weighted + drop * exp_sum), axis=0, keepdims=True), jnp.sum(picked, axis=0, keepdims=True))]
    packed = jnp.zeros((SUBLANES, LANES), jnp.float32)
    for t in range(positions):
        row_max, exp_sum, weighted, picked = wide[t]
        own = lane == t * batch + sub
        top = jnp.max(jnp.where(own, jnp.maximum(row_max, flat[0]), row_max), axis=1, keepdims=True)
        drop, far = row_max - top, jnp.where(own, flat[0] - top, 0.0)
        scale, other = jnp.exp(drop), jnp.exp(far)
        values = (top,
                  jnp.sum(scale * exp_sum + jnp.where(own, other * flat[1], 0.0), axis=1, keepdims=True),
                  jnp.sum(scale * (weighted + drop * exp_sum) + jnp.where(own, other * (flat[2] + far * flat[1]), 0.0), axis=1, keepdims=True),
                  jnp.sum(picked + jnp.where(own, flat[3], 0.0), axis=1, keepdims=True))
        for s, v in enumerate(values):
            packed = jnp.where(lane == s * FIELD + t, v, packed)
    mine_ref[...] = packed
    all_ref[me] = packed
    pl.semaphore_wait(barrier, n - 1)
    copies = []
    for o in order:
        copy = pltpu.make_async_remote_copy(
            src_ref=mine_ref, dst_ref=all_ref.at[me], send_sem=send_sem.at[o], recv_sem=recv_sem.at[o],
            device_id=(group, peers[o]), device_id_type=MESH)
        copy.start()
        copies.append(copy)
    for copy in copies:
        copy.wait()


def combine(n, all_ref, logp_ref, norm_ref, ent_ref):
    parts = [all_ref[d] for d in range(n)]
    fields = [[p if s == 0 else pltpu.roll(p, LANES - s * FIELD, 1) for p in parts] for s in range(4)]
    top = functools.reduce(jnp.maximum, fields[0])
    exp_sum = weighted = picked = jnp.zeros((SUBLANES, LANES), jnp.float32)
    for d in range(n):
        drop = fields[0][d] - top
        scale = jnp.exp(drop)
        exp_sum = exp_sum + scale * fields[1][d]
        weighted = weighted + scale * (fields[2][d] + drop * fields[1][d])
        picked = picked + fields[3][d]
    log_sum = jnp.log(exp_sum)
    log_norm = top + log_sum
    logp_ref[...] = (picked - log_norm)[:, :logp_ref.shape[1]]
    norm_ref[...] = log_norm[:, :norm_ref.shape[1]]
    ent_ref[...] = (log_sum - weighted / exp_sum)[:, :ent_ref.shape[1]]


def solution(mesh):
    n = mesh.shape['tp']

    def per_device(hidden, draft_ids, norm_gain, head_w):
        batch, positions, dim = hidden.shape
        drafts = draft_ids.shape[1]
        rows = batch * positions
        cols = head_w.shape[1]
        x = hidden.transpose(1, 0, 2).reshape(rows, dim)
        gain = norm_gain.reshape(dim // LANES, LANES)
        vmem = pl.BlockSpec(memory_space=pltpu.VMEM)
        hbm = pl.BlockSpec(memory_space=pltpu.HBM)
        f32 = jnp.float32
        padded = pl.cdiv(rows, PACK) * PACK
        partial = pl.pallas_call(
            score,
            out_shape=(jax.ShapeDtypeStruct((4, SUBLANES, LANES), f32),
                       jax.ShapeDtypeStruct((4, positions, SUBLANES, LANES), f32),
                       jax.ShapeDtypeStruct((positions + 1, SUBLANES, LANES), jnp.int32),
                       jax.ShapeDtypeStruct((UNITS, MOVED, LANES), f32),
                       jax.ShapeDtypeStruct((UNITS, padded, UNIT), f32)),
            in_specs=[hbm] * 4,
            out_specs=(vmem,) * 5,
            scratch_shapes=[
                pltpu.VMEM((rows, dim), jnp.bfloat16),
                pltpu.VMEM((batch, drafts), jnp.int32),
                pltpu.VMEM((dim // LANES, LANES), jnp.bfloat16),
                pltpu.VMEM((padded, dim), jnp.bfloat16),
                pltpu.VMEM((dim, LANES), jnp.bfloat16),
                pltpu.VMEM((SLOTS, TRIP, dim), jnp.bfloat16),
                pltpu.VMEM((cols % TRIP, dim), jnp.bfloat16),
                pltpu.SemaphoreType.DMA((3,)),
                pltpu.SemaphoreType.DMA((SLOTS,)),
                pltpu.SemaphoreType.DMA,
                pltpu.SemaphoreType.DMA((CUTS,)),
            ],
            compiler_params=pltpu.CompilerParams(vmem_limit_bytes=SCORE_VMEM),
        )(*[pltpu.with_memory_space_constraint(v, pltpu.HBM) for v in (x, draft_ids, gain, head_w.T)])
        every = pl.pallas_call(
            functools.partial(exchange, n, cols - TRIP),
            out_shape=jax.ShapeDtypeStruct((n, SUBLANES, LANES), f32),
            in_specs=[vmem] * 5,
            out_specs=vmem,
            scratch_shapes=[pltpu.VMEM((SUBLANES, LANES), f32), pltpu.SemaphoreType.DMA((n,)), pltpu.SemaphoreType.DMA((n,))],
            compiler_params=pltpu.CompilerParams(collective_id=0, has_side_effects=True, vmem_limit_bytes=4 * 1024 * 1024),
        )(*partial)
        return pl.pallas_call(
            functools.partial(combine, n),
            out_shape=(jax.ShapeDtypeStruct((batch, drafts), jnp.float32),
                       jax.ShapeDtypeStruct((batch, positions), jnp.float32),
                       jax.ShapeDtypeStruct((batch, positions), jnp.float32)),
            in_specs=[vmem],
            out_specs=(vmem, vmem, vmem),
            compiler_params=pltpu.CompilerParams(vmem_limit_bytes=1024 * 1024),
        )(every)

    specs_in = (P('dp', None, None), P('dp', None), P(None), P(None, 'tp'))
    specs_out = (P('dp', None), P('dp', None), P('dp', None))
    return jax.shard_map(per_device, mesh=mesh, in_specs=specs_in, out_specs=specs_out, check_vma=False)
```

```python
import functools

import jax
import jax.numpy as jnp
from jax import lax
from jax.experimental import pallas as pl
from jax.experimental.pallas import tpu as pltpu
from jax.sharding import PartitionSpec as P

NORM_EPS = 1e-5
MESH = pl.DeviceIdType.MESH
LANES = 128
SUBLANES = 8
UNIT = 256
PACK = 16
HELD = 256
MOVED = 304
UNITS = 2
TRIP = UNITS * (HELD + MOVED)
SLOTS = 4
CUTS = 2
LATE_CUTS = (4, 8)
SCORE_VMEM = 46 * 1024 * 1024
FIELD = 16


def fold(state, tiles, hits, start):
    row_max, exp_sum, weighted, picked = state
    base = row_max if start is None else jnp.where(start, tiles[0], row_max)
    new_max = functools.reduce(jnp.maximum, tiles, base)
    drop = base - new_max
    scale = jnp.exp(drop)
    weighted = scale * (weighted + drop * exp_sum)
    exp_sum = scale * exp_sum
    for tile, hit in zip(tiles, hits):
        shifted = tile - new_max
        exp_vals = jnp.exp(shifted)
        exp_sum = exp_sum + exp_vals
        weighted = weighted + exp_vals * shifted
        picked = picked + jnp.where(hit, tile, 0.0)
    return new_max, exp_sum, weighted, picked


def tall_tiles(logits):
    return [logits[r:r + SUBLANES, :LANES] for r in range(0, logits.shape[0], SUBLANES)]


def tall_hits(tall_ids, first_row, count):
    return [(tall_ids - first_row) == r * SUBLANES for r in range(count)]


def score(x_hbm, ids_hbm, gain_hbm, w_hbm, tall_ref, state_ref, ids_out, moved_ref, held_ref,
          x_ref, ids_ref, gain_ref, n_ref, xt_ref, w_ref, edge_ref, in_sem, w_sem, edge_sem):
    me = lax.axis_index('tp')
    batch, drafts = ids_ref.shape
    rows = x_hbm.shape[0]
    positions = rows // batch
    cols, dim = w_hbm.shape
    depth = dim // UNIT
    trips = cols // TRIP
    edge = cols - trips * TRIP
    late = trips - len(LATE_CUTS)

    def fetch(trip, slot, cuts, c):
        start = pl.multiple_of(edge + trip * TRIP, SUBLANES)
        part = pl.ds(c * (dim // cuts), dim // cuts)
        return pltpu.make_async_copy(w_hbm.at[pl.ds(start, TRIP), part], w_ref.at[slot, :, part], w_sem.at[slot, c])

    def begin(trip, slot, cuts=CUTS):
        for c in range(cuts):
            fetch(trip, slot, cuts, c).start(priority=1)

    inputs = [pltpu.make_async_copy(src, dst, in_sem.at[i])
              for i, (src, dst) in enumerate(((x_hbm, x_ref), (ids_hbm, ids_ref), (gain_hbm, gain_ref)))]
    for copy in inputs:
        copy.start()
    edge_copy = pltpu.make_async_copy(w_hbm.at[pl.ds(0, edge)], edge_ref, edge_sem)
    edge_copy.start()
    for b in range(SLOTS):
        begin(b, b)

    lane = lax.broadcasted_iota(jnp.int32, (SUBLANES, LANES), 1)
    sub = lax.broadcasted_iota(jnp.int32, (SUBLANES, LANES), 0)
    for copy in inputs:
        copy.wait()
    ids = ids_ref[...] - me * cols
    nobody = jnp.full((SUBLANES, LANES), -(1 << 29), jnp.int32)
    wide_ids = [ids[:, t:t + 1] - lane for t in range(drafts)] + [nobody] * (positions - drafts)
    tall_ids = nobody
    for t in range(drafts):
        spread = jnp.sum(jnp.where(lane == t * batch + sub, ids[:, t:t + 1], 0), axis=0, keepdims=True)
        tall_ids = jnp.where(lane // batch == t, spread - sub, tall_ids)

    total = jnp.zeros((rows, LANES), jnp.float32)
    for c in range(dim // LANES):
        wide = x_ref[:, c * LANES:(c + 1) * LANES].astype(jnp.float32)
        total = total + wide * wide
    inv_rms = lax.rsqrt(jnp.sum(total, axis=1, keepdims=True) / dim + NORM_EPS)
    gain = gain_ref[...].astype(jnp.float32)
    pad = jnp.zeros((LANES - rows, LANES), jnp.float32)
    for c in range(dim // LANES):
        wide = x_ref[:, c * LANES:(c + 1) * LANES].astype(jnp.float32)
        normed = jnp.concatenate([wide * inv_rms * gain[c:c + 1, :], pad], axis=0)
        n_ref[:, c * LANES:(c + 1) * LANES] = normed[:n_ref.shape[0]].astype(jnp.bfloat16)
        xt_ref[c * LANES:(c + 1) * LANES, :] = normed.T.astype(jnp.bfloat16)

    zeros = jnp.zeros((UNIT, UNIT - LANES), jnp.bfloat16)

    def hold_x(k, q):
        pltpu.matmul_push_rhs(jnp.concatenate([xt_ref[k * UNIT:(k + 1) * UNIT, :], zeros], axis=1), staging_register=1, mxu_index=q)

    for t in range(positions):
        ids_out[t] = wide_ids[t]
    ids_out[positions] = tall_ids

    def main(held_0, held_1, moved_0, moved_1, edge_0, edge_1):
        held, moved, edges = (held_0, held_1), (moved_0, moved_1), (edge_0, edge_1)
        for ref in held + moved + edges:
            pltpu.matmul_pop(ref)

        half = edge // UNITS
        for q in range(UNITS):
            hold_x(0, q)
        edge_copy.wait()
        for k in range(depth):
            for q in range(UNITS):
                pltpu.matmul_acc_lhs(edges[q], edge_ref[q * half:(q + 1) * half, k * UNIT:(k + 1) * UNIT], load_staged_rhs=1)
                hold_x((k + 1) % depth, q)
        tiles, hits = [], []
        for q in range(UNITS):
            tiles += tall_tiles(pltpu.matmul_pop(edges[q]))
            hits += tall_hits(tall_ids, q * half, half // SUBLANES)
        zero = jnp.zeros((SUBLANES, LANES), jnp.float32)
        tall = fold((tiles[0], zero, zero, zero), tiles, hits, None)
        state_ref[...] = jnp.zeros_like(state_ref)

        def trip_step(trip, slot, tall, cuts=CUTS, last=False):
            first_row = edge + trip * TRIP
            for k in range(depth):
                if k % (depth // cuts) == 0:
                    fetch(trip, slot, cuts, k // (depth // cuts)).wait()
                part = slice(k * UNIT, (k + 1) * UNIT)
                for q in range(UNITS):
                    top = q * (HELD + MOVED)
                    pltpu.matmul_push_rhs(w_ref[slot, top:top + HELD, part], staging_register=0, mxu_index=q, transpose=True)
                    pltpu.matmul_acc_lhs(moved[q], w_ref[slot, top + HELD:top + HELD + MOVED, part], load_staged_rhs=1)
                    if not (last and k == depth - 1):
                        hold_x((k + 1) % depth, q)
                    pltpu.matmul_acc_lhs(held[q], n_ref[:, part], load_staged_rhs=0)
            if last:
                for q in range(UNITS):
                    moved_ref[q] = pltpu.matmul_pop(moved[q])[:, :LANES]
                for q in range(UNITS):
                    held_ref[q] = pltpu.matmul_pop(held[q])
                return tall
            wide_tiles = []
            tiles, hits = [], []
            for q in range(UNITS):
                row = first_row + q * (HELD + MOVED)
                logits = pltpu.matmul_pop(moved[q])
                tiles += tall_tiles(logits)
                hits += tall_hits(tall_ids, row + HELD, MOVED // SUBLANES)
            tall = fold(tall, tiles, hits, None)
            for q in range(UNITS):
                row = first_row + q * (HELD + MOVED)
                logits = pltpu.matmul_pop(held[q])
                for c in range(HELD // LANES):
                    wide_tiles.append((logits[:, c * LANES:(c + 1) * LANES], row + c * LANES))
            for t in range(positions):
                here = slice(t * SUBLANES, (t + 1) * SUBLANES)
                state = tuple(state_ref[s, t] for s in range(4))
                state = fold(state, [z[here] for z, _ in wide_tiles], [wide_ids[t] == row for _, row in wide_tiles], trip == 0)
                for s in range(4):
                    state_ref[s, t] = state[s]
            return tall

        def body(trip, tall):
            slot = lax.rem(trip, SLOTS)
            tall = trip_step(trip, slot, tall)
            ahead = trip + SLOTS

            @pl.when(ahead < late)
            def _():
                begin(ahead, slot)

            for i, cuts in enumerate(LATE_CUTS):
                @pl.when(ahead == late + i)
                def _():
                    begin(late + i, (late + i) % SLOTS, cuts)
            return tall

        tall = lax.fori_loop(0, late, body, tall)
        for i, cuts in enumerate(LATE_CUTS):
            trip = late + i
            tall = trip_step(trip, trip % SLOTS, tall, cuts, trip == trips - 1)

        for s in range(4):
            tall_ref[s] = tall[s]

    acc = pltpu.ACC
    f32 = jnp.float32
    pl.run_scoped(main, *[acc(q)((n_ref.shape[0], UNIT), f32) for q in range(UNITS)],
                  *[acc(q)((MOVED, UNIT), f32) for q in range(UNITS)],
                  *[acc(q)((edge // UNITS, UNIT), f32) for q in range(UNITS)])


def exchange(n, last_row, tall_ref, state_ref, ids_ref, moved_ref, held_ref, all_ref, mine_ref, send_sem, recv_sem):
    me = lax.axis_index('tp')
    group = lax.axis_index('dp')
    batch, positions = SUBLANES, state_ref.shape[1]
    bits = [(d, lax.rem(me // d, 2)) for d in (1, 2, 4)]
    order = [o for o in (6, 7, 4, 5, 2, 3, 1) if o < n]
    peers = {o: me + sum(d * (1 - 2 * b) for d, b in bits if o & d) for o in order}
    barrier = pltpu.get_barrier_semaphore()
    for o in order:
        pl.semaphore_signal(barrier, inc=1, device_id=(group, peers[o]), device_id_type=MESH)

    lane = lax.broadcasted_iota(jnp.int32, (SUBLANES, LANES), 1)
    sub = lax.broadcasted_iota(jnp.int32, (SUBLANES, LANES), 0)
    tiles, hits = [], []
    for q in range(UNITS):
        row = last_row + q * (HELD + MOVED)
        tiles += tall_tiles(moved_ref[q])
        hits += tall_hits(ids_ref[positions], row + HELD, MOVED // SUBLANES)
    tall = fold(tuple(tall_ref[s] for s in range(4)), tiles, hits, None)
    wide = []
    for t in range(positions):
        tiles, hits = [], []
        for q in range(UNITS):
            for c in range(HELD // LANES):
                tiles.append(held_ref[q, t * SUBLANES:(t + 1) * SUBLANES, c * LANES:(c + 1) * LANES])
                hits.append(ids_ref[t] == last_row + q * (HELD + MOVED) + c * LANES)
        wide.append(fold(tuple(state_ref[s, t] for s in range(4)), tiles, hits, None))

    row_max, exp_sum, weighted, picked = tall
    top = jnp.max(row_max, axis=0, keepdims=True)
    drop = row_max - top
    scale = jnp.exp(drop)
    flat = [jnp.broadcast_to(v, (SUBLANES, LANES)) for v in (
        top, jnp.sum(scale * exp_sum, axis=0, keepdims=True),
        jnp.sum(scale * (weighted + drop * exp_sum), axis=0, keepdims=True), jnp.sum(picked, axis=0, keepdims=True))]
    packed = jnp.zeros((SUBLANES, LANES), jnp.float32)
    for t in range(positions):
        row_max, exp_sum, weighted, picked = wide[t]
        own = lane == t * batch + sub
        top = jnp.max(jnp.where(own, jnp.maximum(row_max, flat[0]), row_max), axis=1, keepdims=True)
        drop, far = row_max - top, jnp.where(own, flat[0] - top, 0.0)
        scale, other = jnp.exp(drop), jnp.exp(far)
        values = (top,
                  jnp.sum(scale * exp_sum + jnp.where(own, other * flat[1], 0.0), axis=1, keepdims=True),
                  jnp.sum(scale * (weighted + drop * exp_sum) + jnp.where(own, other * (flat[2] + far * flat[1]), 0.0), axis=1, keepdims=True),
                  jnp.sum(picked + jnp.where(own, flat[3], 0.0), axis=1, keepdims=True))
        for s, v in enumerate(values):
            packed = jnp.where(lane == s * FIELD + t, v, packed)
    mine_ref[...] = packed
    all_ref[me] = packed
    pl.semaphore_wait(barrier, n - 1)
    copies = []
    for o in order:
        copy = pltpu.make_async_remote_copy(
            src_ref=mine_ref, dst_ref=all_ref.at[me], send_sem=send_sem.at[o], recv_sem=recv_sem.at[o],
            device_id=(group, peers[o]), device_id_type=MESH)
        copy.start()
        copies.append(copy)
    for copy in copies:
        copy.wait()


def combine(n, all_ref, logp_ref, norm_ref, ent_ref):
    parts = [all_ref[d] for d in range(n)]
    fields = [[p if s == 0 else pltpu.roll(p, LANES - s * FIELD, 1) for p in parts] for s in range(4)]
    top = functools.reduce(jnp.maximum, fields[0])
    exp_sum = weighted = picked = jnp.zeros((SUBLANES, LANES), jnp.float32)
    for d in range(n):
        drop = fields[0][d] - top
        scale = jnp.exp(drop)
        exp_sum = exp_sum + scale * fields[1][d]
        weighted = weighted + scale * (fields[2][d] + drop * fields[1][d])
        picked = picked + fields[3][d]
    log_sum = jnp.log(exp_sum)
    log_norm = top + log_sum
    logp_ref[...] = (picked - log_norm)[:, :logp_ref.shape[1]]
    norm_ref[...] = log_norm[:, :norm_ref.shape[1]]
    ent_ref[...] = (log_sum - weighted / exp_sum)[:, :ent_ref.shape[1]]


def solution(mesh):
    n = mesh.shape['tp']

    def per_device(hidden, draft_ids, norm_gain, head_w):
        batch, positions, dim = hidden.shape
        drafts = draft_ids.shape[1]
        rows = batch * positions
        cols = head_w.shape[1]
        x = hidden.transpose(1, 0, 2).reshape(rows, dim)
        gain = norm_gain.reshape(dim // LANES, LANES)
        vmem = pl.BlockSpec(memory_space=pltpu.VMEM)
        hbm = pl.BlockSpec(memory_space=pltpu.HBM)
        f32 = jnp.float32
        padded = pl.cdiv(rows, PACK) * PACK
        partial = pl.pallas_call(
            score,
            out_shape=(jax.ShapeDtypeStruct((4, SUBLANES, LANES), f32),
                       jax.ShapeDtypeStruct((4, positions, SUBLANES, LANES), f32),
                       jax.ShapeDtypeStruct((positions + 1, SUBLANES, LANES), jnp.int32),
                       jax.ShapeDtypeStruct((UNITS, MOVED, LANES), f32),
                       jax.ShapeDtypeStruct((UNITS, padded, UNIT), f32)),
            in_specs=[hbm] * 4,
            out_specs=(vmem,) * 5,
            scratch_shapes=[
                pltpu.VMEM((rows, dim), jnp.bfloat16),
                pltpu.VMEM((batch, drafts), jnp.int32),
                pltpu.VMEM((dim // LANES, LANES), jnp.bfloat16),
                pltpu.VMEM((padded, dim), jnp.bfloat16),
                pltpu.VMEM((dim, LANES), jnp.bfloat16),
                pltpu.VMEM((SLOTS, TRIP, dim), jnp.bfloat16),
                pltpu.VMEM((cols % TRIP, dim), jnp.bfloat16),
                pltpu.SemaphoreType.DMA((3,)),
                pltpu.SemaphoreType.DMA((SLOTS, max(CUTS, *LATE_CUTS))),
                pltpu.SemaphoreType.DMA,
            ],
            compiler_params=pltpu.CompilerParams(vmem_limit_bytes=SCORE_VMEM),
        )(*[pltpu.with_memory_space_constraint(v, pltpu.HBM) for v in (x, draft_ids, gain, head_w.T)])
        every = pl.pallas_call(
            functools.partial(exchange, n, cols - TRIP),
            out_shape=jax.ShapeDtypeStruct((n, SUBLANES, LANES), f32),
            in_specs=[vmem] * 5,
            out_specs=vmem,
            scratch_shapes=[pltpu.VMEM((SUBLANES, LANES), f32), pltpu.SemaphoreType.DMA((n,)), pltpu.SemaphoreType.DMA((n,))],
            compiler_params=pltpu.CompilerParams(collective_id=0, has_side_effects=True, vmem_limit_bytes=4 * 1024 * 1024),
        )(*partial)
        return pl.pallas_call(
            functools.partial(combine, n),
            out_shape=(jax.ShapeDtypeStruct((batch, drafts), jnp.float32),
                       jax.ShapeDtypeStruct((batch, positions), jnp.float32),
                       jax.ShapeDtypeStruct((batch, positions), jnp.float32)),
            in_specs=[vmem],
            out_specs=(vmem, vmem, vmem),
            compiler_params=pltpu.CompilerParams(vmem_limit_bytes=1024 * 1024),
        )(every)

    specs_in = (P('dp', None, None), P('dp', None), P(None), P(None, 'tp'))
    specs_out = (P('dp', None), P('dp', None), P('dp', None))
    return jax.shard_map(per_device, mesh=mesh, in_specs=specs_in, out_specs=specs_out, check_vma=False)
```

```python
import functools

import jax
import jax.numpy as jnp
from jax import lax
from jax.experimental import pallas as pl
from jax.experimental.pallas import tpu as pltpu
from jax.sharding import PartitionSpec as P

NORM_EPS = 1e-5
MESH = pl.DeviceIdType.MESH
LANES = 128
SUBLANES = 8
UNIT = 256
PACK = 16
HELD = 256
MOVED = 304
UNITS = 2
TRIP = UNITS * (HELD + MOVED)
SLOTS = 4
CUTS = 2
LATE_CUTS = (4, 4)
SCORE_VMEM = 46 * 1024 * 1024
FIELD = 16


def fold(state, tiles, hits, start):
    row_max, exp_sum, weighted, picked = state
    base = row_max if start is None else jnp.where(start, tiles[0], row_max)
    new_max = functools.reduce(jnp.maximum, tiles, base)
    drop = base - new_max
    scale = jnp.exp(drop)
    weighted = scale * (weighted + drop * exp_sum)
    exp_sum = scale * exp_sum
    for tile, hit in zip(tiles, hits):
        shifted = tile - new_max
        exp_vals = jnp.exp(shifted)
        exp_sum = exp_sum + exp_vals
        weighted = weighted + exp_vals * shifted
        picked = picked + jnp.where(hit, tile, 0.0)
    return new_max, exp_sum, weighted, picked


def tall_tiles(logits):
    return [logits[r:r + SUBLANES, :LANES] for r in range(0, logits.shape[0], SUBLANES)]


def tall_hits(tall_ids, first_row, count):
    return [(tall_ids - first_row) == r * SUBLANES for r in range(count)]


def contract(rows, columns):
    return lax.dot_general(rows, columns, (((1,), (1,)), ((), ())), preferred_element_type=jnp.float32)


def score(n, x_hbm, ids_hbm, gain_hbm, w_hbm, all_ref,
          x_ref, ids_ref, gain_ref, n_ref, xt_ref, w_ref, edge_ref, state_ref, mine_ref,
          in_sem, w_sem, edge_sem, send_sem, recv_sem):
    me = lax.axis_index('tp')
    group = lax.axis_index('dp')
    batch, drafts = ids_ref.shape
    rows = x_hbm.shape[0]
    positions = rows // batch
    cols, dim = w_hbm.shape
    depth = dim // UNIT
    trips = cols // TRIP
    edge = cols - trips * TRIP
    late = trips - len(LATE_CUTS)

    def fetch(trip, slot, cuts, c):
        start = pl.multiple_of(edge + trip * TRIP, SUBLANES)
        part = pl.ds(c * (dim // cuts), dim // cuts)
        return pltpu.make_async_copy(w_hbm.at[pl.ds(start, TRIP), part], w_ref.at[slot, :, part], w_sem.at[slot, c])

    def begin(trip, slot, cuts=CUTS):
        for c in range(cuts):
            fetch(trip, slot, cuts, c).start(priority=1)

    inputs = [pltpu.make_async_copy(src, dst, in_sem.at[i])
              for i, (src, dst) in enumerate(((x_hbm, x_ref), (ids_hbm, ids_ref), (gain_hbm, gain_ref)))]
    for copy in inputs:
        copy.start()
    edge_copy = pltpu.make_async_copy(w_hbm.at[pl.ds(0, edge)], edge_ref, edge_sem)
    edge_copy.start()
    for b in range(SLOTS):
        begin(b, b)

    bits = [(d, lax.rem(me // d, 2)) for d in (1, 2, 4)]
    order = [o for o in (6, 7, 4, 5, 2, 3, 1) if o < n]
    peers = {o: me + sum(d * (1 - 2 * b) for d, b in bits if o & d) for o in order}
    barrier = pltpu.get_barrier_semaphore()
    for o in order:
        pl.semaphore_signal(barrier, inc=1, device_id=(group, peers[o]), device_id_type=MESH)

    for copy in inputs:
        copy.wait()
    lane = lax.broadcasted_iota(jnp.int32, (SUBLANES, LANES), 1)
    sub = lax.broadcasted_iota(jnp.int32, (SUBLANES, LANES), 0)
    ids = ids_ref[...] - me * cols
    nobody = jnp.full((SUBLANES, LANES), -(1 << 29), jnp.int32)
    wide_ids = [ids[:, t:t + 1] - lane for t in range(drafts)] + [nobody] * (positions - drafts)
    tall_ids = nobody
    for t in range(drafts):
        spread = jnp.sum(jnp.where(lane == t * batch + sub, ids[:, t:t + 1], 0), axis=0, keepdims=True)
        tall_ids = jnp.where(lane // batch == t, spread - sub, tall_ids)

    total = jnp.zeros((rows, LANES), jnp.float32)
    for c in range(dim // LANES):
        wide = x_ref[:, c * LANES:(c + 1) * LANES].astype(jnp.float32)
        total = total + wide * wide
    inv_rms = lax.rsqrt(jnp.sum(total, axis=1, keepdims=True) / dim + NORM_EPS)
    gain = gain_ref[...].astype(jnp.float32)
    pad = jnp.zeros((LANES - rows, LANES), jnp.float32)
    for c in range(dim // LANES):
        wide = x_ref[:, c * LANES:(c + 1) * LANES].astype(jnp.float32)
        normed = jnp.concatenate([wide * inv_rms * gain[c:c + 1, :], pad], axis=0)
        n_ref[:, c * LANES:(c + 1) * LANES] = normed[:n_ref.shape[0]].astype(jnp.bfloat16)
        xt_ref[c * LANES:(c + 1) * LANES, :] = normed.T.astype(jnp.bfloat16)
    state_ref[...] = jnp.zeros_like(state_ref)

    def trip_step(trip, slot, tall, cuts=CUTS):
        moved, held = [0.0] * UNITS, [0.0] * UNITS
        for k in range(depth):
            if k % (depth // cuts) == 0:
                fetch(trip, slot, cuts, k // (depth // cuts)).wait()
            part = slice(k * UNIT, (k + 1) * UNIT)
            for q in range(UNITS):
                top = q * (HELD + MOVED)
                moved[q] += jnp.dot(w_ref[slot, top + HELD:top + HELD + MOVED, part], xt_ref[part, :], preferred_element_type=jnp.float32)
                held[q] += contract(n_ref[:, part], w_ref[slot, top:top + HELD, part])
        tiles, hits, wide = [], [], []
        for q in range(UNITS):
            row = edge + trip * TRIP + q * (HELD + MOVED)
            tiles += tall_tiles(moved[q])
            hits += tall_hits(tall_ids, row + HELD, MOVED // SUBLANES)
            wide += [(held[q][:, c:c + LANES], row + c) for c in range(0, HELD, LANES)]
        tall = fold(tall, tiles, hits, None)
        for t in range(positions):
            here = slice(t * SUBLANES, (t + 1) * SUBLANES)
            state = tuple(state_ref[s, t] for s in range(4))
            state = fold(state, [z[here] for z, _ in wide], [wide_ids[t] == row for _, row in wide], trip == 0)
            for s in range(4):
                state_ref[s, t] = state[s]
        return tall

    def body(trip, tall):
        slot = lax.rem(trip, SLOTS)
        tall = trip_step(trip, slot, tall)
        ahead = trip + SLOTS

        @pl.when(ahead < late)
        def _():
            begin(ahead, slot)

        for i, cuts in enumerate(LATE_CUTS):
            @pl.when(ahead == late + i)
            def _():
                begin(late + i, (late + i) % SLOTS, cuts)
        return tall

    zero = jnp.zeros((SUBLANES, LANES), jnp.float32)
    half = edge // UNITS
    logits = [0.0] * UNITS
    edge_copy.wait()
    for k in range(depth):
        part = slice(k * UNIT, (k + 1) * UNIT)
        for q in range(UNITS):
            logits[q] += jnp.dot(edge_ref[q * half:(q + 1) * half, part], xt_ref[part, :], preferred_element_type=jnp.float32)
    tiles, hits = [], []
    for q in range(UNITS):
        tiles += tall_tiles(logits[q])
        hits += tall_hits(tall_ids, q * half, half // SUBLANES)
    tall = fold((tiles[0], zero, zero, zero), tiles, hits, None)
    tall = lax.fori_loop(0, late, body, tall)
    for i, cuts in enumerate(LATE_CUTS):
        tall = trip_step(late + i, (late + i) % SLOTS, tall, cuts)

    columns = {}
    for t in range(positions):
        row_max, exp_sum, weighted, picked = (state_ref[s, t] for s in range(4))
        top = jnp.max(row_max, axis=1, keepdims=True)
        drop = row_max - top
        scale = jnp.exp(drop)
        for s, v in enumerate((None, scale * exp_sum, scale * (weighted + drop * exp_sum), picked)):
            columns[s, t] = top if s == 0 else jnp.sum(v, axis=1, keepdims=True)

    row_max, exp_sum, weighted, picked = tall

    top = jnp.max(row_max, axis=0, keepdims=True)
    drop = row_max - top
    scale = jnp.exp(drop)
    flat = (top, jnp.sum(scale * exp_sum, axis=0, keepdims=True),
            jnp.sum(scale * (weighted + drop * exp_sum), axis=0, keepdims=True), jnp.sum(picked, axis=0, keepdims=True))
    for s, v in enumerate(flat):
        for t in range(positions):
            columns[s + 4, t] = jnp.sum(jnp.where(lane == t * batch + sub, v, 0.0), axis=1, keepdims=True)
    packed = zero
    for (s, t), v in columns.items():
        packed = jnp.where(lane == s * FIELD + t, v, packed)
    all_ref[me] = packed
    mine_ref[...] = packed

    pl.semaphore_wait(barrier, n - 1)
    copies = []
    for o in order:
        copy = pltpu.make_async_remote_copy(
            src_ref=mine_ref, dst_ref=all_ref.at[me], send_sem=send_sem.at[o], recv_sem=recv_sem.at[o],
            device_id=(group, peers[o]), device_id_type=MESH)
        copy.start()
        copies.append(copy)
    for copy in copies:
        copy.wait()


def combine(all_ref, logp_ref, norm_ref, ent_ref):
    tiles = [all_ref[d] for d in range(all_ref.shape[0])]
    parts = [[tile if s == 0 else pltpu.roll(tile, LANES - s * FIELD, 1) for s in range(first, first + 4)] for first in (0, 4) for tile in tiles]
    top = functools.reduce(jnp.maximum, [part[0] for part in parts])
    exp_sum = weighted = picked = jnp.zeros((SUBLANES, LANES), jnp.float32)
    for row_max, sums, products, found in parts:
        drop = row_max - top
        scale = jnp.exp(drop)
        exp_sum = exp_sum + scale * sums
        weighted = weighted + scale * (products + drop * sums)
        picked = picked + found
    log_sum = jnp.log(exp_sum)
    log_norm = top + log_sum
    logp_ref[...] = (picked - log_norm)[:, :logp_ref.shape[1]]
    norm_ref[...] = log_norm[:, :norm_ref.shape[1]]
    ent_ref[...] = (log_sum - weighted / exp_sum)[:, :ent_ref.shape[1]]


def solution(mesh):
    n = mesh.shape['tp']

    def per_device(hidden, draft_ids, norm_gain, head_w):
        batch, positions, dim = hidden.shape
        drafts = draft_ids.shape[1]
        rows = batch * positions
        cols = head_w.shape[1]
        x = hidden.transpose(1, 0, 2).reshape(rows, dim)
        gain = norm_gain.reshape(dim // LANES, LANES)
        vmem = pl.BlockSpec(memory_space=pltpu.VMEM)
        hbm = pl.BlockSpec(memory_space=pltpu.HBM)
        f32 = jnp.float32
        padded = pl.cdiv(rows, PACK) * PACK
        every = pl.pallas_call(
            functools.partial(score, n),
            out_shape=jax.ShapeDtypeStruct((n, SUBLANES, LANES), f32),
            in_specs=[hbm] * 4,
            out_specs=vmem,
            scratch_shapes=[
                pltpu.VMEM((rows, dim), jnp.bfloat16),
                pltpu.VMEM((batch, drafts), jnp.int32),
                pltpu.VMEM((dim // LANES, LANES), jnp.bfloat16),
                pltpu.VMEM((padded, dim), jnp.bfloat16),
                pltpu.VMEM((dim, LANES), jnp.bfloat16),
                pltpu.VMEM((SLOTS, TRIP, dim), jnp.bfloat16),
                pltpu.VMEM((cols % TRIP, dim), jnp.bfloat16),
                pltpu.VMEM((4, positions, SUBLANES, LANES), f32),
                pltpu.VMEM((SUBLANES, LANES), f32),
                pltpu.SemaphoreType.DMA((3,)),
                pltpu.SemaphoreType.DMA((SLOTS, max(CUTS, *LATE_CUTS))),
                pltpu.SemaphoreType.DMA,
                pltpu.SemaphoreType.DMA((n,)),
                pltpu.SemaphoreType.DMA((n,)),
            ],
            compiler_params=pltpu.CompilerParams(collective_id=0, has_side_effects=True, vmem_limit_bytes=SCORE_VMEM),
        )(*[pltpu.with_memory_space_constraint(v, pltpu.HBM) for v in (x, draft_ids, gain, head_w.T)])
        return pl.pallas_call(
            combine,
            out_shape=(jax.ShapeDtypeStruct((batch, drafts), jnp.float32),
                       jax.ShapeDtypeStruct((batch, positions), jnp.float32),
                       jax.ShapeDtypeStruct((batch, positions), jnp.float32)),
            in_specs=[vmem],
            out_specs=(vmem, vmem, vmem),
            compiler_params=pltpu.CompilerParams(vmem_limit_bytes=1024 * 1024),
        )(every)

    specs_in = (P('dp', None, None), P('dp', None), P(None), P(None, 'tp'))
    specs_out = (P('dp', None), P('dp', None), P('dp', None))
    return jax.shard_map(per_device, mesh=mesh, in_specs=specs_in, out_specs=specs_out, check_vma=False)
```

```python
import functools

import jax
import jax.numpy as jnp
from jax import lax
from jax.experimental import pallas as pl
from jax.experimental.pallas import tpu as pltpu
from jax.sharding import PartitionSpec as P

NORM_EPS = 1e-5
MESH = pl.DeviceIdType.MESH
LANES = 128
SUBLANES = 8
UNIT = 256
PACK = 16
HELD = 256
MOVED = 272
UNITS = 2
TRIP = UNITS * (HELD + MOVED)
SLOTS = 3
CUTS = (8, 8)
LATE_CUTS = ((6, 5, 5), (6, 5, 3, 2))
SCORE_VMEM = 46 * 1024 * 1024
FIELD = 16


def fold(state, tiles, hits, start):
    row_max, exp_sum, weighted, picked = state
    base = row_max if start is None else jnp.where(start, tiles[0], row_max)
    new_max = functools.reduce(jnp.maximum, tiles, base)
    drop = base - new_max
    scale = jnp.exp(drop)
    weighted = scale * (weighted + drop * exp_sum)
    exp_sum = scale * exp_sum
    for tile, hit in zip(tiles, hits):
        shifted = tile - new_max
        exp_vals = jnp.exp(shifted)
        exp_sum = exp_sum + exp_vals
        weighted = weighted + exp_vals * shifted
        picked = picked + jnp.where(hit, tile, 0.0)
    return new_max, exp_sum, weighted, picked


def tall_tiles(logits):
    return [logits[r:r + SUBLANES, :LANES] for r in range(0, logits.shape[0], SUBLANES)]


def tall_hits(tall_ids, first_row, count):
    return [(tall_ids - first_row) == r * SUBLANES for r in range(count)]


def contract(rows, columns):
    return lax.dot_general(rows, columns, (((1,), (1,)), ((), ())), preferred_element_type=jnp.float32)


def score(n, x_hbm, ids_hbm, gain_hbm, w_hbm, all_ref,
          x_ref, ids_ref, gain_ref, n_ref, xt_ref, w_ref, edge_ref, state_ref, mine_ref,
          in_sem, w_sem, edge_sem, send_sem, recv_sem):
    me = lax.axis_index('tp')
    group = lax.axis_index('dp')
    batch, drafts = ids_ref.shape
    rows = x_hbm.shape[0]
    positions = rows // batch
    cols, dim = w_hbm.shape
    depth = dim // UNIT
    trips = cols // TRIP
    edge = cols - trips * TRIP
    late = trips - len(LATE_CUTS)

    def fetch(trip, slot, cuts, c):
        start = pl.multiple_of(edge + trip * TRIP, SUBLANES)
        part = pl.ds(sum(cuts[:c]) * UNIT, cuts[c] * UNIT)
        return pltpu.make_async_copy(w_hbm.at[pl.ds(start, TRIP), part], w_ref.at[slot, :, part], w_sem.at[slot, c])

    def begin(trip, slot, cuts=CUTS):
        for c in range(len(cuts)):
            fetch(trip, slot, cuts, c).start(priority=1)

    inputs = [pltpu.make_async_copy(src, dst, in_sem.at[i])
              for i, (src, dst) in enumerate(((x_hbm, x_ref), (ids_hbm, ids_ref), (gain_hbm, gain_ref)))]
    for copy in inputs:
        copy.start()
    edge_copy = pltpu.make_async_copy(w_hbm.at[pl.ds(0, edge)], edge_ref, edge_sem)
    edge_copy.start()
    for b in range(SLOTS):
        begin(b, b)

    bits = [(d, lax.rem(me // d, 2)) for d in (1, 2, 4)]
    order = [o for o in (6, 7, 4, 5, 2, 3, 1) if o < n]
    peers = {o: me + sum(d * (1 - 2 * b) for d, b in bits if o & d) for o in order}
    barrier = pltpu.get_barrier_semaphore()
    for o in order:
        pl.semaphore_signal(barrier, inc=1, device_id=(group, peers[o]), device_id_type=MESH)

    for copy in inputs:
        copy.wait()
    lane = lax.broadcasted_iota(jnp.int32, (SUBLANES, LANES), 1)
    sub = lax.broadcasted_iota(jnp.int32, (SUBLANES, LANES), 0)
    ids = ids_ref[...] - me * cols
    nobody = jnp.full((SUBLANES, LANES), -(1 << 29), jnp.int32)
    wide_ids = [ids[:, t:t + 1] - lane for t in range(drafts)] + [nobody] * (positions - drafts)
    tall_ids = nobody
    for t in range(drafts):
        spread = jnp.sum(jnp.where(lane == t * batch + sub, ids[:, t:t + 1], 0), axis=0, keepdims=True)
        tall_ids = jnp.where(lane // batch == t, spread - sub, tall_ids)

    total = jnp.zeros((rows, LANES), jnp.float32)
    for c in range(dim // LANES):
        wide = x_ref[:, c * LANES:(c + 1) * LANES].astype(jnp.float32)
        total = total + wide * wide
    inv_rms = lax.rsqrt(jnp.sum(total, axis=1, keepdims=True) / dim + NORM_EPS)
    gain = gain_ref[...].astype(jnp.float32)
    pad = jnp.zeros((LANES - rows, LANES), jnp.float32)
    for c in range(dim // LANES):
        wide = x_ref[:, c * LANES:(c + 1) * LANES].astype(jnp.float32)
        normed = jnp.concatenate([wide * inv_rms * gain[c:c + 1, :], pad], axis=0)
        n_ref[:, c * LANES:(c + 1) * LANES] = normed[:n_ref.shape[0]].astype(jnp.bfloat16)
        xt_ref[c * LANES:(c + 1) * LANES, :] = normed.T.astype(jnp.bfloat16)
    state_ref[...] = jnp.zeros_like(state_ref)

    def trip_step(trip, slot, tall, cuts=CUTS):
        moved, held = [0.0] * UNITS, [0.0] * UNITS
        for k in range(depth):
            for c in range(len(cuts)):
                if k == sum(cuts[:c]):
                    fetch(trip, slot, cuts, c).wait()
            part = slice(k * UNIT, (k + 1) * UNIT)
            for q in range(UNITS):
                top = q * (HELD + MOVED)
                moved[q] += jnp.dot(w_ref[slot, top + HELD:top + HELD + MOVED, part], xt_ref[part, :], preferred_element_type=jnp.float32)
                held[q] += contract(n_ref[:, part], w_ref[slot, top:top + HELD, part])
        tiles, hits, wide = [], [], []
        for q in range(UNITS):
            row = edge + trip * TRIP + q * (HELD + MOVED)
            tiles += tall_tiles(moved[q])
            hits += tall_hits(tall_ids, row + HELD, MOVED // SUBLANES)
            wide += [(held[q][:, c:c + LANES], row + c) for c in range(0, HELD, LANES)]
        tall = fold(tall, tiles, hits, None)
        for t in range(positions):
            here = slice(t * SUBLANES, (t + 1) * SUBLANES)
            state = tuple(state_ref[s, t] for s in range(4))
            state = fold(state, [z[here] for z, _ in wide], [wide_ids[t] == row for _, row in wide], trip == 0)
            for s in range(4):
                state_ref[s, t] = state[s]
        return tall

    def body(trip, tall):
        slot = lax.rem(trip, SLOTS)
        tall = trip_step(trip, slot, tall)
        ahead = trip + SLOTS

        @pl.when(ahead < late)
        def _():
            begin(ahead, slot)

        for i, cuts in enumerate(LATE_CUTS):
            @pl.when(ahead == late + i)
            def _():
                begin(late + i, (late + i) % SLOTS, cuts)
        return tall

    zero = jnp.zeros((SUBLANES, LANES), jnp.float32)
    half = edge // UNITS
    logits = [0.0] * UNITS
    edge_copy.wait()
    for k in range(depth):
        part = slice(k * UNIT, (k + 1) * UNIT)
        for q in range(UNITS):
            logits[q] += jnp.dot(edge_ref[q * half:(q + 1) * half, part], xt_ref[part, :], preferred_element_type=jnp.float32)
    tiles, hits = [], []
    for q in range(UNITS):
        tiles += tall_tiles(logits[q])
        hits += tall_hits(tall_ids, q * half, half // SUBLANES)
    tall = fold((tiles[0], zero, zero, zero), tiles, hits, None)
    tall = lax.fori_loop(0, late, body, tall)
    for i, cuts in enumerate(LATE_CUTS):
        tall = trip_step(late + i, (late + i) % SLOTS, tall, cuts)

    columns = {}
    for t in range(positions):
        row_max, exp_sum, weighted, picked = (state_ref[s, t] for s in range(4))
        top = jnp.max(row_max, axis=1, keepdims=True)
        drop = row_max - top
        scale = jnp.exp(drop)
        for s, v in enumerate((None, scale * exp_sum, scale * (weighted + drop * exp_sum), picked)):
            columns[s, t] = top if s == 0 else jnp.sum(v, axis=1, keepdims=True)

    row_max, exp_sum, weighted, picked = tall

    top = jnp.max(row_max, axis=0, keepdims=True)
    drop = row_max - top
    scale = jnp.exp(drop)
    flat = (top, jnp.sum(scale * exp_sum, axis=0, keepdims=True),
            jnp.sum(scale * (weighted + drop * exp_sum), axis=0, keepdims=True), jnp.sum(picked, axis=0, keepdims=True))
    for s, v in enumerate(flat):
        for t in range(positions):
            columns[s + 4, t] = jnp.sum(jnp.where(lane == t * batch + sub, v, 0.0), axis=1, keepdims=True)
    packed = zero
    for (s, t), v in columns.items():
        packed = jnp.where(lane == s * FIELD + t, v, packed)
    all_ref[me] = packed
    mine_ref[...] = packed

    pl.semaphore_wait(barrier, n - 1)
    copies = []
    for o in order:
        copy = pltpu.make_async_remote_copy(
            src_ref=mine_ref, dst_ref=all_ref.at[me], send_sem=send_sem.at[o], recv_sem=recv_sem.at[o],
            device_id=(group, peers[o]), device_id_type=MESH)
        copy.start()
        copies.append(copy)
    for copy in copies:
        copy.wait()


def combine(all_ref, logp_ref, norm_ref, ent_ref):
    tiles = [all_ref[d] for d in range(all_ref.shape[0])]
    parts = [[tile if s == 0 else pltpu.roll(tile, LANES - s * FIELD, 1) for s in range(first, first + 4)] for first in (0, 4) for tile in tiles]
    top = functools.reduce(jnp.maximum, [part[0] for part in parts])
    exp_sum = weighted = picked = jnp.zeros((SUBLANES, LANES), jnp.float32)
    for row_max, sums, products, found in parts:
        drop = row_max - top
        scale = jnp.exp(drop)
        exp_sum = exp_sum + scale * sums
        weighted = weighted + scale * (products + drop * sums)
        picked = picked + found
    log_sum = jnp.log(exp_sum)
    log_norm = top + log_sum
    logp_ref[...] = (picked - log_norm)[:, :logp_ref.shape[1]]
    norm_ref[...] = log_norm[:, :norm_ref.shape[1]]
    ent_ref[...] = (log_sum - weighted / exp_sum)[:, :ent_ref.shape[1]]


def solution(mesh):
    n = mesh.shape['tp']

    def per_device(hidden, draft_ids, norm_gain, head_w):
        batch, positions, dim = hidden.shape
        drafts = draft_ids.shape[1]
        rows = batch * positions
        cols = head_w.shape[1]
        x = hidden.transpose(1, 0, 2).reshape(rows, dim)
        gain = norm_gain.reshape(dim // LANES, LANES)
        vmem = pl.BlockSpec(memory_space=pltpu.VMEM)
        hbm = pl.BlockSpec(memory_space=pltpu.HBM)
        f32 = jnp.float32
        padded = pl.cdiv(rows, PACK) * PACK
        every = pl.pallas_call(
            functools.partial(score, n),
            out_shape=jax.ShapeDtypeStruct((n, SUBLANES, LANES), f32),
            in_specs=[hbm] * 4,
            out_specs=vmem,
            scratch_shapes=[
                pltpu.VMEM((rows, dim), jnp.bfloat16),
                pltpu.VMEM((batch, drafts), jnp.int32),
                pltpu.VMEM((dim // LANES, LANES), jnp.bfloat16),
                pltpu.VMEM((padded, dim), jnp.bfloat16),
                pltpu.VMEM((dim, LANES), jnp.bfloat16),
                pltpu.VMEM((SLOTS, TRIP, dim), jnp.bfloat16),
                pltpu.VMEM((cols % TRIP, dim), jnp.bfloat16),
                pltpu.VMEM((4, positions, SUBLANES, LANES), f32),
                pltpu.VMEM((SUBLANES, LANES), f32),
                pltpu.SemaphoreType.DMA((3,)),
                pltpu.SemaphoreType.DMA((SLOTS, max(map(len, (CUTS, *LATE_CUTS))))),
                pltpu.SemaphoreType.DMA,
                pltpu.SemaphoreType.DMA((n,)),
                pltpu.SemaphoreType.DMA((n,)),
            ],
            compiler_params=pltpu.CompilerParams(collective_id=0, has_side_effects=True, vmem_limit_bytes=SCORE_VMEM),
        )(*[pltpu.with_memory_space_constraint(v, pltpu.HBM) for v in (x, draft_ids, gain, head_w.T)])
        return pl.pallas_call(
            combine,
            out_shape=(jax.ShapeDtypeStruct((batch, drafts), jnp.float32),
                       jax.ShapeDtypeStruct((batch, positions), jnp.float32),
                       jax.ShapeDtypeStruct((batch, positions), jnp.float32)),
            in_specs=[vmem],
            out_specs=(vmem, vmem, vmem),
            compiler_params=pltpu.CompilerParams(vmem_limit_bytes=1024 * 1024),
        )(every)

    specs_in = (P('dp', None, None), P('dp', None), P(None), P(None, 'tp'))
    specs_out = (P('dp', None), P('dp', None), P('dp', None))
    return jax.shard_map(per_device, mesh=mesh, in_specs=specs_in, out_specs=specs_out, check_vma=False)
```

```python
import functools

import jax
import jax.numpy as jnp
from jax import lax
from jax.experimental import pallas as pl
from jax.experimental.pallas import tpu as pltpu
from jax.sharding import PartitionSpec as P

NORM_EPS = 1e-5
MESH = pl.DeviceIdType.MESH
LANES = 128
SUBLANES = 8
UNIT = 256
PACK = 16
HELD = 256
MOVED = 272
UNITS = 2
TRIP = UNITS * (HELD + MOVED)
SLOTS = 3
CUTS = (8, 8)
LATE_CUTS = ((6, 5, 5), (6, 5, 3, 2))
SCORE_VMEM = 46 * 1024 * 1024
FIELD = 16


def fold(state, tiles, hits, start):
    row_max, exp_sum, weighted, picked = state
    base = row_max if start is None else jnp.where(start, tiles[0], row_max)
    new_max = functools.reduce(jnp.maximum, tiles, base)
    drop = base - new_max
    scale = jnp.exp(drop)
    weighted = scale * (weighted + drop * exp_sum)
    exp_sum = scale * exp_sum
    for tile, hit in zip(tiles, hits):
        shifted = tile - new_max
        exp_vals = jnp.exp(shifted)
        exp_sum = exp_sum + exp_vals
        weighted = weighted + exp_vals * shifted
        picked = picked + jnp.where(hit, tile, 0.0)
    return new_max, exp_sum, weighted, picked


def tall_tiles(logits):
    return [logits[r:r + SUBLANES, :LANES] for r in range(0, logits.shape[0], SUBLANES)]


def tall_hits(tall_ids, first_row, count):
    return [(tall_ids - first_row) == r * SUBLANES for r in range(count)]


def contract(rows, columns):
    return lax.dot_general(rows, columns, (((1,), (1,)), ((), ())), preferred_element_type=jnp.float32)


def score(n, x_hbm, ids_hbm, gain_hbm, w_hbm, all_ref,
          x_ref, ids_ref, gain_ref, n_ref, xt_ref, w_ref, edge_ref, state_ref, mine_ref,
          in_sem, w_sem, edge_sem, send_sem, recv_sem):
    me = lax.axis_index('tp')
    group = lax.axis_index('dp')
    batch, drafts = ids_ref.shape
    rows = x_hbm.shape[0]
    positions = rows // batch
    cols, dim = w_hbm.shape
    depth = dim // UNIT
    trips = cols // TRIP
    edge = cols - trips * TRIP
    late = trips - len(LATE_CUTS)

    def fetch(trip, slot, cuts, c):
        start = pl.multiple_of(edge + trip * TRIP, SUBLANES)
        part = pl.ds(sum(cuts[:c]) * UNIT, cuts[c] * UNIT)
        return pltpu.make_async_copy(w_hbm.at[pl.ds(start, TRIP), part], w_ref.at[slot, :, part], w_sem.at[slot, c])

    def begin(trip, slot, cuts=CUTS):
        for c in range(len(cuts)):
            fetch(trip, slot, cuts, c).start(priority=1)

    inputs = [pltpu.make_async_copy(src, dst, in_sem.at[i])
              for i, (src, dst) in enumerate(((x_hbm, x_ref), (ids_hbm, ids_ref), (gain_hbm, gain_ref)))]
    for copy in inputs:
        copy.start()
    edge_copy = pltpu.make_async_copy(w_hbm.at[pl.ds(0, edge)], edge_ref, edge_sem)
    edge_copy.start()
    for b in range(SLOTS):
        begin(b, b)

    bits = [(d, lax.rem(me // d, 2)) for d in (1, 2, 4)]
    order = [o for o in (6, 7, 4, 5, 2, 3, 1) if o < n]
    peers = {o: me + sum(d * (1 - 2 * b) for d, b in bits if o & d) for o in order}
    barrier = pltpu.get_barrier_semaphore()
    for o in order:
        pl.semaphore_signal(barrier, inc=1, device_id=(group, peers[o]), device_id_type=MESH)

    for copy in inputs:
        copy.wait()
    lane = lax.broadcasted_iota(jnp.int32, (SUBLANES, LANES), 1)
    sub = lax.broadcasted_iota(jnp.int32, (SUBLANES, LANES), 0)
    ids = ids_ref[...] - me * cols
    nobody = jnp.full((SUBLANES, LANES), -(1 << 29), jnp.int32)
    wide_ids = [ids[:, t:t + 1] - lane for t in range(drafts)] + [nobody] * (positions - drafts)
    tall_ids = nobody
    for t in range(drafts):
        spread = jnp.sum(jnp.where(lane == t * batch + sub, ids[:, t:t + 1], 0), axis=0, keepdims=True)
        tall_ids = jnp.where(lane // batch == t, spread - sub, tall_ids)

    total = jnp.zeros((rows, LANES), jnp.float32)
    for c in range(dim // LANES):
        wide = x_ref[:, c * LANES:(c + 1) * LANES].astype(jnp.float32)
        total = total + wide * wide
    inv_rms = lax.rsqrt(jnp.sum(total, axis=1, keepdims=True) / dim + NORM_EPS)
    gain = gain_ref[...].astype(jnp.float32)
    pad = jnp.zeros((LANES - rows, LANES), jnp.float32)
    for c in range(dim // LANES):
        wide = x_ref[:, c * LANES:(c + 1) * LANES].astype(jnp.float32)
        normed = jnp.concatenate([wide * inv_rms * gain[c:c + 1, :], pad], axis=0)
        n_ref[:, c * LANES:(c + 1) * LANES] = normed[:n_ref.shape[0]].astype(jnp.bfloat16)
        xt_ref[c * LANES:(c + 1) * LANES, :] = normed.T.astype(jnp.bfloat16)
    state_ref[...] = jnp.zeros_like(state_ref)

    def trip_step(trip, slot, tall, cuts=CUTS):
        moved, held = [0.0] * UNITS, [0.0] * UNITS
        for k in range(depth):
            for c in range(len(cuts)):
                if k == sum(cuts[:c]):
                    fetch(trip, slot, cuts, c).wait()
            part = slice(k * UNIT, (k + 1) * UNIT)
            for q in range(UNITS):
                top = q * (HELD + MOVED)
                moved[q] += jnp.dot(w_ref[slot, top + HELD:top + HELD + MOVED, part], xt_ref[part, :], preferred_element_type=jnp.float32)
                held[q] += contract(n_ref[:, part], w_ref[slot, top:top + HELD, part])
        tiles, hits, wide = [], [], []
        for q in range(UNITS):
            row = edge + trip * TRIP + q * (HELD + MOVED)
            tiles += tall_tiles(moved[q])
            hits += tall_hits(tall_ids, row + HELD, MOVED // SUBLANES)
            wide += [(held[q][:, c:c + LANES], row + c) for c in range(0, HELD, LANES)]
        tall = fold(tall, tiles, hits, None)
        for t in range(positions):
            here = slice(t * SUBLANES, (t + 1) * SUBLANES)
            state = tuple(state_ref[s, t] for s in range(4))
            state = fold(state, [z[here] for z, _ in wide], [wide_ids[t] == row for _, row in wide], trip == 0)
            for s in range(4):
                state_ref[s, t] = state[s]
        return tall

    def body(trip, tall):
        slot = lax.rem(trip, SLOTS)
        tall = trip_step(trip, slot, tall)
        ahead = trip + SLOTS

        @pl.when(ahead < late)
        def _():
            begin(ahead, slot)

        for i, cuts in enumerate(LATE_CUTS):
            @pl.when(ahead == late + i)
            def _():
                begin(late + i, (late + i) % SLOTS, cuts)
        return tall

    zero = jnp.zeros((SUBLANES, LANES), jnp.float32)
    half = edge // UNITS
    logits = [0.0] * UNITS
    edge_copy.wait()
    for k in range(depth):
        part = slice(k * UNIT, (k + 1) * UNIT)
        for q in range(UNITS):
            logits[q] += jnp.dot(edge_ref[q * half:(q + 1) * half, part], xt_ref[part, :], preferred_element_type=jnp.float32)
    tiles, hits = [], []
    for q in range(UNITS):
        tiles += tall_tiles(logits[q])
        hits += tall_hits(tall_ids, q * half, half // SUBLANES)
    tall = fold((tiles[0], zero, zero, zero), tiles, hits, None)
    tall = lax.fori_loop(0, late, body, tall)
    for i, cuts in enumerate(LATE_CUTS):
        tall = trip_step(late + i, (late + i) % SLOTS, tall, cuts)

    columns = {}
    for t in range(positions):
        row_max, exp_sum, weighted, picked = (state_ref[s, t] for s in range(4))
        top = jnp.max(row_max, axis=1, keepdims=True)
        drop = row_max - top
        scale = jnp.exp(drop)
        for s, v in enumerate((None, scale * exp_sum, scale * (weighted + drop * exp_sum), picked)):
            columns[s, t] = top if s == 0 else jnp.sum(v, axis=1, keepdims=True)

    row_max, exp_sum, weighted, picked = tall

    top = jnp.max(row_max, axis=0, keepdims=True)
    drop = row_max - top
    scale = jnp.exp(drop)
    flat = (top, jnp.sum(scale * exp_sum, axis=0, keepdims=True),
            jnp.sum(scale * (weighted + drop * exp_sum), axis=0, keepdims=True), jnp.sum(picked, axis=0, keepdims=True))
    packed = zero
    for s in range(4):
        spread = zero
        for t in range(positions):
            spread = jnp.where(lane == t * batch + sub, columns[s, t], spread)
        packed = jnp.where(sub == s, flat[s], jnp.where(sub == s + 4, jnp.sum(spread, axis=0, keepdims=True), packed))
    all_ref[me] = packed
    mine_ref[...] = packed

    pl.semaphore_wait(barrier, n - 1)
    copies = []
    for o in order:
        copy = pltpu.make_async_remote_copy(
            src_ref=mine_ref, dst_ref=all_ref.at[me], send_sem=send_sem.at[o], recv_sem=recv_sem.at[o],
            device_id=(group, peers[o]), device_id_type=MESH)
        copy.start()
        copies.append(copy)
    for copy in copies:
        copy.wait()


def combine(all_ref, logp_ref, norm_ref, ent_ref):
    parts = [[all_ref[:, s, :] for s in range(first, first + 4)] for first in (0, 4)]
    top = functools.reduce(jnp.maximum, [jnp.max(part[0], axis=0, keepdims=True) for part in parts])
    exp_sum = weighted = picked = jnp.zeros((all_ref.shape[0], LANES), jnp.float32)
    for row_max, sums, products, found in parts:
        drop = row_max - top
        scale = jnp.exp(drop)
        exp_sum = exp_sum + scale * sums
        weighted = weighted + scale * (products + drop * sums)
        picked = picked + found
    exp_sum, weighted, picked = (jnp.sum(v, axis=0, keepdims=True) for v in (exp_sum, weighted, picked))
    log_sum = jnp.log(exp_sum)
    log_norm = top + log_sum
    lane = lax.broadcasted_iota(jnp.int32, (SUBLANES, LANES), 1)
    sub = lax.broadcasted_iota(jnp.int32, (SUBLANES, LANES), 0)
    for ref, values in ((logp_ref, picked - log_norm), (norm_ref, log_norm), (ent_ref, log_sum - weighted / exp_sum)):
        out = jnp.zeros((SUBLANES, LANES), jnp.float32)
        for t in range(ref.shape[1]):
            column = jnp.sum(jnp.where(lane == t * SUBLANES + sub, values, 0.0), axis=1, keepdims=True)
            out = jnp.where(lane == t, column, out)
        ref[...] = out[:, :ref.shape[1]]


def solution(mesh):
    n = mesh.shape['tp']

    def per_device(hidden, draft_ids, norm_gain, head_w):
        batch, positions, dim = hidden.shape
        drafts = draft_ids.shape[1]
        rows = batch * positions
        cols = head_w.shape[1]
        x = hidden.transpose(1, 0, 2).reshape(rows, dim)
        gain = norm_gain.reshape(dim // LANES, LANES)
        vmem = pl.BlockSpec(memory_space=pltpu.VMEM)
        hbm = pl.BlockSpec(memory_space=pltpu.HBM)
        f32 = jnp.float32
        padded = pl.cdiv(rows, PACK) * PACK
        every = pl.pallas_call(
            functools.partial(score, n),
            out_shape=jax.ShapeDtypeStruct((n, SUBLANES, LANES), f32),
            in_specs=[hbm] * 4,
            out_specs=vmem,
            scratch_shapes=[
                pltpu.VMEM((rows, dim), jnp.bfloat16),
                pltpu.VMEM((batch, drafts), jnp.int32),
                pltpu.VMEM((dim // LANES, LANES), jnp.bfloat16),
                pltpu.VMEM((padded, dim), jnp.bfloat16),
                pltpu.VMEM((dim, LANES), jnp.bfloat16),
                pltpu.VMEM((SLOTS, TRIP, dim), jnp.bfloat16),
                pltpu.VMEM((cols % TRIP, dim), jnp.bfloat16),
                pltpu.VMEM((4, positions, SUBLANES, LANES), f32),
                pltpu.VMEM((SUBLANES, LANES), f32),
                pltpu.SemaphoreType.DMA((3,)),
                pltpu.SemaphoreType.DMA((SLOTS, max(map(len, (CUTS, *LATE_CUTS))))),
                pltpu.SemaphoreType.DMA,
                pltpu.SemaphoreType.DMA((n,)),
                pltpu.SemaphoreType.DMA((n,)),
            ],
            compiler_params=pltpu.CompilerParams(collective_id=0, has_side_effects=True, vmem_limit_bytes=SCORE_VMEM),
        )(*[pltpu.with_memory_space_constraint(v, pltpu.HBM) for v in (x, draft_ids, gain, head_w.T)])
        return pl.pallas_call(
            combine,
            out_shape=(jax.ShapeDtypeStruct((batch, drafts), jnp.float32),
                       jax.ShapeDtypeStruct((batch, positions), jnp.float32),
                       jax.ShapeDtypeStruct((batch, positions), jnp.float32)),
            in_specs=[vmem],
            out_specs=(vmem, vmem, vmem),
            compiler_params=pltpu.CompilerParams(vmem_limit_bytes=1024 * 1024),
        )(every)

    specs_in = (P('dp', None, None), P('dp', None), P(None), P(None, 'tp'))
    specs_out = (P('dp', None), P('dp', None), P('dp', None))
    return jax.shard_map(per_device, mesh=mesh, in_specs=specs_in, out_specs=specs_out, check_vma=False)
```
